32 devices in a mesh: dp: 4 (over y, x), expert: 8 (over z, core).
Axes of the slice: x: 2, y: 2, z: 4, core: 2. Of those that a mesh axis runs over, the one named last changes fastest.
Arguments:
- tokens: bfloat16 [4096, 2048], P(('dp', 'expert')), may hold values from -6 to 6
- cotangent: bfloat16 [4096, 2048], P(('dp', 'expert')), may hold values from -6 to 6
- attention_norm_gain: float32 [2048], replicated, may hold values from 0.25 to 1.75
- experts_norm_gain: float32 [2048], replicated, may hold values from 0.25 to 1.75
- attention_query_key_value: bfloat16 [2048, 6144], P(None, 'expert'), may hold values from -0.125 to 0.125
- attention_output_weight: bfloat16 [2048, 2048], P('expert'), may hold values from -2 to 2
- router_projection: bfloat16 [2048, 8], replicated, may hold values from -0.0625 to 0.0625
- shared_gate_up_weight: bfloat16 [2, 2048, 5632], P(None, None, 'expert'), may hold values from -0.125 to 0.125
- shared_down_weight: bfloat16 [5632, 2048], P('expert'), may hold values from -0.078125 to 0.078125
- shared_gate_vector: bfloat16 [2048], replicated, may hold values from -0.125 to 0.125
- expert_gate_up_weight: bfloat16 [8, 2, 2048, 1408], P('expert'), may hold values from -0.125 to 0.125
- expert_down_weight: bfloat16 [8, 1408, 2048], P('expert'), may hold values from -0.15625 to 0.15625
- routes: int32 [4096, 4], P(('dp', 'expert')), may hold values from 0 to 7, all different within a row; in each aligned block of 128 rows (0 to 127, 128 to 255, ...) at most 72 rows name the same one
- lengths: int32 [4], P('dp'), may hold values from 256 to 1024, as said below
- adapter_slot_index: int32 [4], P('dp'), may hold values from 0 to 7
- attention_adapter_first: bfloat16 [4, 2048, 128], replicated, may hold values from -0.125 to 0.125
- attention_adapter_second: bfloat16 [4, 128, 2048], replicated, may hold values from -0.75 to 0.75
- router_adapter_first: bfloat16 [2048, 128], replicated, may hold values from -0.125 to 0.125
- router_adapter_second: bfloat16 [128, 8], replicated, may hold values from -0.375 to 0.375
- shared_adapter_first: bfloat16 [2, 2048, 128], replicated, may hold values from -0.125 to 0.125
- shared_adapter_second: bfloat16 [2, 128, 5632], replicated, may hold values from -0.75 to 0.75
- shared_down_adapter_first: bfloat16 [5632, 128], replicated, may hold values from -0.078125 to 0.078125
- shared_down_adapter_second: bfloat16 [128, 2048], replicated, may hold values from -0.75 to 0.75
- expert_adapter_first: bfloat16 [8, 2, 2048, 128], P('expert'), may hold values from -0.125 to 0.125
- expert_adapter_second: bfloat16 [8, 2, 128, 1408], P('expert'), may hold values from -0.75 to 0.75
- expert_down_adapter_first: bfloat16 [8, 1408, 128], P('expert'), may hold values from -0.15625 to 0.15625
- expert_down_adapter_second: bfloat16 [8, 128, 2048], P('expert'), may hold values from -0.75 to 0.75
Outputs:
- layer_out: bfloat16 [4096, 2048], P(('dp', 'expert'))
- tokens_grad: float32 [4096, 2048], P(('dp', 'expert'))
- grad_attn_lora_a: float32 [4, 2048, 128], P(None, None, ('dp', 'expert'))
- grad_attn_lora_b: float32 [4, 128, 2048], P(None, ('dp', 'expert'))
- grad_router_lora_a: float32 [2048, 128], P(None, ('dp', 'expert'))
- grad_router_lora_b: float32 [128, 8], P(('dp', 'expert'))
- grad_shared_lora_a: float32 [2, 2048, 128], P(None, None, ('dp', 'expert'))
- grad_shared_lora_b: float32 [2, 128, 5632], P(None, ('dp', 'expert'))
- grad_shared_down_lora_a: float32 [5632, 128], P(None, ('dp', 'expert'))
- grad_shared_down_lora_b: float32 [128, 2048], P(('dp', 'expert'))
- grad_expert_lora_a: float32 [8, 2, 2048, 128], P('expert')
- grad_expert_lora_b: float32 [8, 2, 128, 1408], P('expert')
- grad_expert_down_lora_a: float32 [8, 1408, 128], P('expert')
- grad_expert_down_lora_b: float32 [8, 128, 2048], P('expert')
The draws below stay inside these ranges and needn't reach their ends.
Inputs may be any that keep to these rules, and one draw needn't show every extreme that they name: `routes`: each row names 4 different experts. Among the rows of one device no expert is named more than 72 times, and in some device's rows one expert is named exactly 72 times. `lengths`: one sequence slot keeps all 1024 tokens in every draw.
All inputs are finite; a program needn't handle non-finite values.
Results may differ from the reference program's by a relative error of at most 0.02.
Values may be sent and summed in bfloat16 or wider, within the bound.
A program may use at most 512 MiB of HBM per device.

```python
import math
import jax
import jax.numpy as jnp
import numpy as np
from jax import lax

MODEL_DIM = 2048
HEADS = 16
HEAD_DIM = 128
EXPERT_FEEDWIDE = 1408
SHARED_FEEDWIDE = 5632
TOP = 4
ADAPTER_RANK = 16
ADAPTER_COUNT = 8
BLOCK = 256
TOK_DEV = 128
EXPERT_COUNT = 8
SEQ_LEN = 1024
TOKENS = 4096
SEQS = 4
CAP = 72


def draw_lengths(key, part):
    first_key, second_key = jax.random.split(key)
    values = jax.random.randint(first_key, (SEQS,), BLOCK, SEQ_LEN + 1)
    full_slot = jax.random.randint(second_key, (), 0, SEQS)
    return jnp.where(jnp.arange(SEQS) == full_slot, SEQ_LEN, values).astype(jnp.int32)


def with_ends(array, own_key, least, top_value):
    dims = array.shape
    index_at = [jax.random.randint(jax.random.fold_in(own_key, axis), (), 0, dims[axis]) for axis in range(len(dims))]
    array = array.at[tuple(index_at)].set(least)
    longest = dims.index(max(dims))
    index_at[longest] = (index_at[longest] + 1) % dims[longest]
    return array.at[tuple(index_at)].set(top_value)


def levels(rng, dims, pieces, low, high):
    level = 1.0
    for axis_at, parts in pieces:
        draws = jax.random.uniform(jax.random.fold_in(jax.random.fold_in(rng, 6), axis_at), (parts,), jnp.float32, low / len(pieces), high / len(pieces))
        level = level * jnp.repeat(jnp.exp(draws), dims[axis_at] // parts).reshape((-1,) + (1,) * (len(dims) - 1 - axis_at))
    return level


def routed_block(key, own, number, rows, count, top, limit, skew):
    ranking = jax.random.permutation(key, count)
    heavy_load, usual = load_shares(count, rows * top, limit, skew, True), load_shares(count, rows * top, limit, skew, False)
    places = jnp.arange(count)

    def named(sizes, rotation):
        used = int((sizes > 0).sum())
        fixed = max(1, used // 4)
        passed = fixed + (places - fixed + rotation * (used - fixed)) % max(1, count - fixed)
        return jnp.zeros((count,), jnp.int32).at[ranking[jnp.where(places < fixed, places, passed)]].set(jnp.asarray(sizes, jnp.int32))

    sizes = jnp.where(number % 4 == 0, named(heavy_load, number // 4), named(usual, number - number // 4 - 1))
    mixed = jax.random.permutation(jax.random.fold_in(own, 3), count)
    source_of, sink = mixed[0:count // 2 * 2:2], mixed[1:count // 2 * 2:2]
    room = jnp.minimum(sizes[source_of] - 1, limit - sizes[sink]) // 2
    room = jnp.where((source_of == ranking[0]) | (sink == ranking[0]) | (sizes[sink] == 0), 0, jnp.maximum(room, 0))
    passed = jax.random.randint(jax.random.fold_in(own, 4), (count // 2,), 0, 1 << 20) % (room + 1)
    sizes = sizes.at[source_of].add(-passed).at[sink].add(passed)
    members = jnp.searchsorted(jnp.cumsum(sizes), jnp.arange(rows * top), side="right").astype(jnp.int32)
    grid = members.reshape(top, rows).T
    grid = grid[jax.random.permutation(jax.random.fold_in(own, 1), rows)]
    rotation = jax.random.randint(jax.random.fold_in(own, 2), (rows, 1), 0, top)
    return jnp.take_along_axis(grid, (jnp.arange(top)[None, :] + rotation) % top, axis=1)


def load_shares(count, total, reach, slope, full):
    weights = [(1 << 20) // math.isqrt(standing ** slope) + 1 for standing in range(1, count + 1)]
    largest = reach if full else min(reach, max(-(-total // count), total * weights[0] // sum(weights)))
    least = 1 if total - largest >= count - 1 else 0
    holding, rest = [largest] + [least] * (count - 1), total - largest - least * (count - 1)
    while rest > 0:
        free = [i for i in range(1, count) if holding[i] < largest] or [i for i in range(1, count) if holding[i] < reach]
        whole, budget = sum([weights[i] for i in free]), rest
        for i in free:
            more = min(reach - holding[i], max(1, budget * weights[i] // whole), rest)
            holding[i] = holding[i] + more
            rest = rest - more
    return np.array(holding)


def gaussian(key, dims, deviation, reach, pieces=(), kind=jnp.bfloat16):
    level = levels(key, dims, pieces, -0.22, 0.18) if pieces else 1.0
    result = jax.random.normal(key, dims, jnp.float32) * deviation * level
    return jnp.minimum(jnp.maximum(result, -reach), reach).astype(kind)


def setup_inputs(seed: int = 0) -> dict:
    streams_of = jax.random.split(jax.random.key(seed), 28)
    tokens = gaussian(streams_of[0], (TOKENS, MODEL_DIM), 1.0, 6.0, ((0, 32),))
    cotangent = gaussian(streams_of[1], (TOKENS, MODEL_DIM), 1.0, 6.0, ((0, 32),))
    attention_norm_gain = jnp.clip(1.0 + 0.15 * jax.random.normal(streams_of[2], (MODEL_DIM,), jnp.float32), 0.25, 1.75)
    experts_norm_gain = jnp.clip(1.0 + 0.15 * jax.random.normal(streams_of[3], (MODEL_DIM,), jnp.float32), 0.25, 1.75)
    attention_query_key_value = gaussian(streams_of[4], (MODEL_DIM, 3 * MODEL_DIM), MODEL_DIM ** -0.5, 0.125, ((1, 8),))
    attention_output_weight = gaussian(streams_of[5], (MODEL_DIM, MODEL_DIM), (max(MODEL_DIM // 256, 1)) ** -0.5, 2.0, ((0, 8),))
    router_projection = gaussian(streams_of[6], (MODEL_DIM, EXPERT_COUNT), (4 * MODEL_DIM) ** -0.5, 0.0625)
    shared_gate_up_weight = gaussian(streams_of[7], (2, MODEL_DIM, SHARED_FEEDWIDE), MODEL_DIM ** -0.5, 0.125, ((2, 8),))
    shared_down_weight = gaussian(streams_of[8], (SHARED_FEEDWIDE, MODEL_DIM), SHARED_FEEDWIDE ** -0.5, 0.078125, ((0, 8),))
    shared_gate_vector = gaussian(streams_of[9], (MODEL_DIM,), MODEL_DIM ** -0.5, 0.125)
    expert_gate_up_weight = gaussian(streams_of[10], (EXPERT_COUNT, 2, MODEL_DIM, EXPERT_FEEDWIDE), MODEL_DIM ** -0.5, 0.125, ((0, 8),))
    expert_down_weight = gaussian(streams_of[11], (EXPERT_COUNT, EXPERT_FEEDWIDE, MODEL_DIM), EXPERT_FEEDWIDE ** -0.5, 0.15625, ((0, 8),))
    routes_keys = jax.random.split(jax.random.fold_in(streams_of[12], 1), TOKENS // TOK_DEV)
    routes_turns = jax.random.permutation(jax.random.fold_in(streams_of[12], 3), TOKENS // TOK_DEV)
    routes = jax.vmap(lambda own, number: routed_block(jax.random.fold_in(streams_of[12], 2), own, number, TOK_DEV, EXPERT_COUNT, TOP, CAP, 2))(routes_keys, routes_turns).reshape((TOKENS, TOP))
    lengths = draw_lengths(jax.random.fold_in(streams_of[27], 71), 0)
    adapter_slot_index = with_ends(jax.random.randint(streams_of[14], (SEQS,), 0, ADAPTER_COUNT), jax.random.fold_in(streams_of[14], 1), 0, ADAPTER_COUNT - 1).astype(jnp.int32)
    attention_adapter_first = gaussian(streams_of[15], (4, MODEL_DIM, ADAPTER_COUNT * ADAPTER_RANK), MODEL_DIM ** -0.5, 0.125)
    attention_adapter_second = gaussian(streams_of[16], (4, ADAPTER_COUNT * ADAPTER_RANK, MODEL_DIM), (4 * ADAPTER_RANK) ** -0.5, 0.75)
    router_adapter_first = gaussian(streams_of[17], (MODEL_DIM, ADAPTER_COUNT * ADAPTER_RANK), MODEL_DIM ** -0.5, 0.125)
    router_adapter_second = gaussian(streams_of[18], (ADAPTER_COUNT * ADAPTER_RANK, EXPERT_COUNT), (16 * ADAPTER_RANK) ** -0.5, 0.375)
    shared_adapter_first = gaussian(streams_of[19], (2, MODEL_DIM, ADAPTER_COUNT * ADAPTER_RANK), MODEL_DIM ** -0.5, 0.125)
    shared_adapter_second = gaussian(streams_of[20], (2, ADAPTER_COUNT * ADAPTER_RANK, SHARED_FEEDWIDE), (4 * ADAPTER_RANK) ** -0.5, 0.75)
    shared_down_adapter_first = gaussian(streams_of[21], (SHARED_FEEDWIDE, ADAPTER_COUNT * ADAPTER_RANK), SHARED_FEEDWIDE ** -0.5, 0.078125)
    shared_down_adapter_second = gaussian(streams_of[22], (ADAPTER_COUNT * ADAPTER_RANK, MODEL_DIM), (4 * ADAPTER_RANK) ** -0.5, 0.75)
    expert_adapter_first = gaussian(streams_of[23], (EXPERT_COUNT, 2, MODEL_DIM, ADAPTER_COUNT * ADAPTER_RANK), MODEL_DIM ** -0.5, 0.125, ((0, 8),))
    expert_adapter_second = gaussian(streams_of[24], (EXPERT_COUNT, 2, ADAPTER_COUNT * ADAPTER_RANK, EXPERT_FEEDWIDE), (4 * ADAPTER_RANK) ** -0.5, 0.75, ((0, 8),))
    expert_down_adapter_first = gaussian(streams_of[25], (EXPERT_COUNT, EXPERT_FEEDWIDE, ADAPTER_COUNT * ADAPTER_RANK), EXPERT_FEEDWIDE ** -0.5, 0.15625, ((0, 8),))
    expert_down_adapter_second = gaussian(streams_of[26], (EXPERT_COUNT, ADAPTER_COUNT * ADAPTER_RANK, MODEL_DIM), (4 * ADAPTER_RANK) ** -0.5, 0.75, ((0, 8),))
    return {"tokens": tokens, "cotangent": cotangent, "attention_norm_gain": attention_norm_gain, "experts_norm_gain": experts_norm_gain, "attention_query_key_value": attention_query_key_value, "attention_output_weight": attention_output_weight, "router_projection": router_projection, "shared_gate_up_weight": shared_gate_up_weight, "shared_down_weight": shared_down_weight, "shared_gate_vector": shared_gate_vector, "expert_gate_up_weight": expert_gate_up_weight, "expert_down_weight": expert_down_weight, "routes": routes, "lengths": lengths, "adapter_slot_index": adapter_slot_index, "attention_adapter_first": attention_adapter_first, "attention_adapter_second": attention_adapter_second, "router_adapter_first": router_adapter_first, "router_adapter_second": router_adapter_second, "shared_adapter_first": shared_adapter_first, "shared_adapter_second": shared_adapter_second, "shared_down_adapter_first": shared_down_adapter_first, "shared_down_adapter_second": shared_down_adapter_second, "expert_adapter_first": expert_adapter_first, "expert_adapter_second": expert_adapter_second, "expert_down_adapter_first": expert_down_adapter_first, "expert_down_adapter_second": expert_down_adapter_second}


@jax.custom_vjp
def low(v):
    return lax.optimization_barrier(v.astype(jnp.bfloat16)).astype(jnp.float32)

@jax.custom_vjp
def narrow_backward(v):
    return v

def low_keep(v):
    return (low(v), None)

def low_pass(kept, grad):
    return (grad,)

def back_keep(v):
    return (v, None)

def back_low(kept, grad):
    return (low(grad),)
low.defvjp(low_keep, low_pass)
narrow_backward.defvjp(back_keep, back_low)
HIGHEST_PRECISION = lax.Precision.HIGHEST
NORM_EPS = 1e-06
ROPE_BASE = 1000000.0
MASKED = -1e+30

def matrix_product(left_side, right_side):
    return jnp.dot(left_side, right_side, precision=HIGHEST_PRECISION, preferred_element_type=jnp.float32)

def rms_norm(values, gain_vector):
    return values * lax.rsqrt(lax.optimization_barrier(jnp.mean(values * values, axis=-1, keepdims=True)) + NORM_EPS) * gain_vector

def adapter_choice(input_rows, down_map, up_map, slot_picker):
    inner_value = low(narrow_backward(slot_picker * matrix_product(input_rows, down_map)))
    return matrix_product(inner_value, up_map)

def rope_tables(positions, head_width):
    half_width = head_width // 2
    inverse = ROPE_BASE ** (-(jnp.arange(half_width).astype(jnp.float32) * 2.0 / head_width))
    angles = positions.astype(jnp.float32)[:, None] * inverse[None, :]
    return (jnp.cos(angles), jnp.sin(angles))

def rotate(values, cosine_table, sine_table, direction):
    half_width = values.shape[-1] // 2
    first_half = values[..., :half_width]
    second_half = values[..., half_width:]
    cosine_part = cosine_table[:, None, :]
    sine_part = sine_table[:, None, :] * direction
    return jnp.concatenate([first_half * cosine_part - second_half * sine_part, second_half * cosine_part + first_half * sine_part], axis=-1)

def reference(tokens, cotangent, attention_norm_gain, experts_norm_gain, attention_query_key_value, attention_output_weight, router_projection, shared_gate_up_weight, shared_down_weight, shared_gate_vector, expert_gate_up_weight, expert_down_weight, routes, lengths, adapter_slot_index, attention_adapter_first, attention_adapter_second, router_adapter_first, router_adapter_second, shared_adapter_first, shared_adapter_second, shared_down_adapter_first, shared_down_adapter_second, expert_adapter_first, expert_adapter_second, expert_down_adapter_first, expert_down_adapter_second):
    token_total = TOKENS
    model_width_size = MODEL_DIM
    columns = ADAPTER_COUNT * ADAPTER_RANK
    token_index = jnp.arange(token_total, dtype=jnp.int32)
    sequence = token_index // SEQ_LEN
    position = token_index % SEQ_LEN
    chosen = adapter_slot_index[sequence].astype(jnp.int32)
    slot_picker = (jnp.arange(columns, dtype=jnp.int32)[None, :] // ADAPTER_RANK == chosen[:, None]).astype(jnp.float32)
    cosine_table, sine_table = rope_tables(position, HEAD_DIM)
    local_index = jnp.arange(SEQ_LEN, dtype=jnp.int32)
    local_block = local_index // BLOCK
    score_scale = 1.0 / math.sqrt(HEAD_DIM)
    flat_routes = routes.reshape(-1).astype(jnp.int32)
    flat_rows = token_total * TOP
    route_hits = (flat_routes[:, None] == jnp.arange(EXPERT_COUNT, dtype=jnp.int32)[None, :]).astype(jnp.int32)
    slot_ranks = lax.optimization_barrier(jnp.sum((jnp.cumsum(route_hits, axis=0).astype(jnp.int32) - 1) * route_hits, axis=1)).astype(jnp.int32)
    most_rows = TOKENS // TOK_DEV * CAP
    row_table = jnp.full((EXPERT_COUNT, most_rows), flat_rows, jnp.int32).at[flat_routes, slot_ranks].set(jnp.arange(flat_rows, dtype=jnp.int32))
    token_lookup = (row_table // TOP).astype(jnp.int32)
    qkv_weight = attention_query_key_value.astype(jnp.float32)
    projection_matrix = attention_output_weight.astype(jnp.float32)
    router_single_float = router_projection.astype(jnp.float32)
    shared_single_float = shared_gate_up_weight.astype(jnp.float32)
    shared_down_single = shared_down_weight.astype(jnp.float32)
    shared_gate_float = shared_gate_vector.astype(jnp.float32)
    seq_shape = (SEQS, SEQ_LEN, HEADS, HEAD_DIM)

    def attention(queries, key_rows, value_rows):

        def one_sequence(block_item):
            query_block, key_block, value_block, key_live = block_item
            raw_scores = narrow_backward(jnp.einsum('qhd,khd->hqk', query_block, key_block, precision=HIGHEST_PRECISION) * score_scale)
            allowed = (local_block[None, :] <= local_block[:, None]) & (local_index[None, :] < key_live)
            weights = low(jax.nn.softmax(jnp.where(allowed[None], raw_scores, MASKED), axis=-1))
            return jnp.einsum('hqk,khd->qhd', weights, value_block, precision=HIGHEST_PRECISION)
        attention_result = lax.map(jax.checkpoint(one_sequence), (queries.reshape(seq_shape), key_rows.reshape(seq_shape), value_rows.reshape(seq_shape), lengths))
        return attention_result.reshape(token_total, model_width_size)

    def forward_pass(input_rows, adapter_attention_first, adapter_attention_second, adapter_router_first, adapter_router_second, adapter_shared_first, adapter_shared_second, adapter_shared_down_first, adapter_shared_down_second, adapter_expert_first, adapter_expert_second, adapter_expert_down_first, adapter_expert_down_second):
        first_narrow = low(rms_norm(input_rows, attention_norm_gain))
        query_key_value_product = matrix_product(first_narrow, qkv_weight)
        preactivation_portions = [query_key_value_product[:, portion_index * model_width_size:(portion_index + 1) * model_width_size] + adapter_choice(first_narrow, adapter_attention_first[portion_index], adapter_attention_second[portion_index], slot_picker) for portion_index in range(3)]
        head_shape = (token_total, HEADS, HEAD_DIM)
        queries = low(rotate(narrow_backward(preactivation_portions[0]).reshape(head_shape), cosine_table, sine_table, 1.0))
        key_rows = low(rotate(narrow_backward(preactivation_portions[1]).reshape(head_shape), cosine_table, sine_table, 1.0))
        value_rows = low(narrow_backward(preactivation_portions[2])).reshape(head_shape)
        attention_result = low(narrow_backward(attention(queries, key_rows, value_rows)))
        residual_stream = input_rows + narrow_backward(matrix_product(attention_result, projection_matrix) + adapter_choice(attention_result, adapter_attention_first[3], adapter_attention_second[3], slot_picker))
        second_factor = low(rms_norm(residual_stream, experts_norm_gain))
        router_scores = narrow_backward(matrix_product(second_factor, router_single_float) + adapter_choice(second_factor, adapter_router_first, adapter_router_second, slot_picker))
        gate_weights = jax.nn.softmax(jnp.take_along_axis(router_scores, routes, axis=1), axis=1)
        padded_rows = jnp.concatenate([second_factor, jnp.zeros((1, model_width_size), jnp.float32)], axis=0)
        padded_selector = jnp.concatenate([slot_picker, jnp.zeros((1, columns), jnp.float32)], axis=0)

        def expert_choice(block_item):
            rows_index, gate_up, down_proj, in_a, in_b, out_a, out_b = block_item
            expert_input_rows = narrow_backward(padded_rows[rows_index])
            row_selector = padded_selector[rows_index]
            gate_up_float = gate_up.astype(jnp.float32)
            gate_value = narrow_backward(matrix_product(expert_input_rows, gate_up_float[0]) + adapter_choice(expert_input_rows, in_a[0], in_b[0], row_selector))
            up_value = narrow_backward(matrix_product(expert_input_rows, gate_up_float[1]) + adapter_choice(expert_input_rows, in_a[1], in_b[1], row_selector))
            hidden = low(jax.nn.silu(gate_value) * up_value)
            return low(narrow_backward(matrix_product(hidden, down_proj.astype(jnp.float32)) + adapter_choice(hidden, out_a, out_b, row_selector)))
        produced_output = lax.map(jax.checkpoint(expert_choice), (token_lookup, expert_gate_up_weight, expert_down_weight, adapter_expert_first, adapter_expert_second, adapter_expert_down_first, adapter_expert_down_second))
        placed = jnp.zeros((flat_rows + 1, model_width_size), jnp.float32).at[row_table.reshape(-1)].add(produced_output.reshape(-1, model_width_size))
        routed = placed[:flat_rows].reshape(token_total, TOP, model_width_size)
        mixture = lax.optimization_barrier(jnp.sum(gate_weights[:, :, None] * routed, axis=1))
        shared_gate_amount = narrow_backward(matrix_product(second_factor, shared_single_float[0]) + adapter_choice(second_factor, adapter_shared_first[0], adapter_shared_second[0], slot_picker))
        shared_up_amount = narrow_backward(matrix_product(second_factor, shared_single_float[1]) + adapter_choice(second_factor, adapter_shared_first[1], adapter_shared_second[1], slot_picker))
        shared_hidden_units = low(jax.nn.silu(shared_gate_amount) * shared_up_amount)
        shared_output_value = narrow_backward(matrix_product(shared_hidden_units, shared_down_single) + adapter_choice(shared_hidden_units, adapter_shared_down_first, adapter_shared_down_second, slot_picker))
        shared_weight = jax.nn.sigmoid(jnp.dot(second_factor, shared_gate_float, precision=HIGHEST_PRECISION))
        return residual_stream + mixture + shared_weight[:, None] * shared_output_value
    final_result, pullback_function = jax.vjp(forward_pass, tokens.astype(jnp.float32), attention_adapter_first.astype(jnp.float32), attention_adapter_second.astype(jnp.float32), router_adapter_first.astype(jnp.float32), router_adapter_second.astype(jnp.float32), shared_adapter_first.astype(jnp.float32), shared_adapter_second.astype(jnp.float32), shared_down_adapter_first.astype(jnp.float32), shared_down_adapter_second.astype(jnp.float32), expert_adapter_first.astype(jnp.float32), expert_adapter_second.astype(jnp.float32), expert_down_adapter_first.astype(jnp.float32), expert_down_adapter_second.astype(jnp.float32))
    gradients = pullback_function(cotangent.astype(jnp.float32))
    return (final_result.astype(jnp.bfloat16), gradients[0], gradients[1], gradients[2], gradients[3], gradients[4], gradients[5], gradients[6], gradients[7], gradients[8], gradients[9], gradients[10], gradients[11], gradients[12])
```

```python
import math

import jax
import jax.numpy as jnp
from jax import lax
from jax.sharding import PartitionSpec as P

HEADS = 16
HEAD_DIM = 128
ADAPTER_RANK = 16
ADAPTER_COUNT = 8
BLOCK = 256
SEQ_MAX = 2048


NORM_EPS = 1e-06
ROPE_BASE = 1000000.0
MASKED = -1e30


def narrow_product(left_side, right_side):
    return jnp.dot(left_side, right_side, preferred_element_type=jnp.float32)


def rms_forward(values, gain_vector):
    factor = lax.rsqrt(jnp.mean(values * values, axis=-1, keepdims=True) + NORM_EPS)
    return (values * factor * gain_vector, factor)


def rms_backward(values, factor, gain_vector, upstream):
    weighted = upstream * gain_vector
    return factor * weighted - values * (factor * factor * factor) * jnp.mean(
        values * weighted, axis=-1, keepdims=True
    )


def rope_tables(positions, head_width):
    half_width = head_width // 2
    inverse = ROPE_BASE ** (-(jnp.arange(half_width).astype(jnp.float32) * 2.0 / head_width))
    angles = positions.astype(jnp.float32)[:, None] * inverse[None, :]
    return (jnp.cos(angles), jnp.sin(angles))


def rotate(values, cosine_table, sine_table, direction):
    half_width = values.shape[-1] // 2
    first_half = values[..., :half_width]
    second_half = values[..., half_width:]
    cosine_part = cosine_table[:, None, :]
    sine_part = sine_table[:, None, :] * direction
    return jnp.concatenate(
        [
            first_half * cosine_part - second_half * sine_part,
            second_half * cosine_part + first_half * sine_part,
        ],
        axis=-1,
    )


def rows_product(left_side, right_side):
    return lax.dot_general(
        left_side, right_side, (((1,), (1,)), ((), ())), preferred_element_type=jnp.float32
    )


def token_product(left_side, right_side):
    return lax.dot_general(
        left_side, right_side, (((0,), (0,)), ((), ())), preferred_element_type=jnp.float32
    )


def gated_back(gate_value, up_value, grad_hidden):
    sigmoid_gate = jax.nn.sigmoid(gate_value)
    grad_gate = grad_hidden * up_value * sigmoid_gate * (1.0 + gate_value * (1.0 - sigmoid_gate))
    grad_up = grad_hidden * gate_value * sigmoid_gate
    return (grad_gate.astype(jnp.bfloat16), grad_up.astype(jnp.bfloat16))


def head_weights(columns, owner_index, owners, slot_count, head_start, width):
    model_width_size, held = columns.shape
    if slot_count == 1 and held == 3 * width and owners % 3:
        moved = [
            lax.ppermute(
                columns[:, step * width : (step + 1) * width],
                "expert",
                [(source, (3 * source + step) % owners) for source in range(owners)],
            )
            for step in range(3)
        ]
        stacked = jnp.stack(moved)
        return jnp.stack(
            [
                lax.dynamic_index_in_dim(stacked, (owner_index + owners * kind) % 3, 0, False)
                for kind in range(3)
            ]
        )
    full = lax.all_gather(columns, "expert", axis=1, tiled=True)
    return jnp.stack(
        [
            lax.dynamic_slice_in_dim(full, kind * model_width_size + head_start * HEAD_DIM, width, 1)
            for kind in range(3)
        ]
    )


def spread_adapters(compact, adapter_index):
    ranks = ADAPTER_COUNT * ADAPTER_RANK
    total = jnp.zeros((ranks, compact.shape[1]), compact.dtype)
    for slot in range(adapter_index.shape[0]):
        piece = compact[slot * ADAPTER_RANK : (slot + 1) * ADAPTER_RANK]
        total = total + lax.dynamic_update_slice_in_dim(
            jnp.zeros_like(total), piece, adapter_index[slot] * ADAPTER_RANK, 0
        )
    return total


def reduce_adapters(
    partial, owned, owned_starts, owned_totals, adapter_index, adapter_groups, owner_index, owners
):
    groups = lax.axis_size("dp")
    group_index = lax.axis_index("dp")
    slot_count = adapter_index.shape[0]
    partial_sizes = [value.shape[1] for value in partial]
    owned_sizes = [value.shape[1] for value in owned]
    partial_all = jnp.concatenate(partial, axis=1)
    owned_all = jnp.concatenate(owned, axis=1)

    def cut(values, sizes):
        pieces, at = [], 0
        for size in sizes:
            pieces.append(values[..., at : at + size])
            at += size
        return pieces

    if slot_count > 1 or ADAPTER_RANK % owners or ADAPTER_COUNT % groups or owners % (
        ADAPTER_COUNT // groups
    ):
        wide = [
            lax.dynamic_update_slice_in_dim(
                jnp.zeros((value.shape[0], total), value.dtype), value, start, 1
            )
            for value, start, total in zip(owned, owned_starts, owned_totals)
        ]
        dense = spread_adapters(jnp.concatenate([partial_all] + wide, axis=1), adapter_index)
        summed = lax.psum_scatter(dense, ("dp", "expert"), scatter_dimension=0, tiled=True)
        pieces = cut(summed, partial_sizes + owned_totals)
        return pieces[: len(partial)], pieces[len(partial) :]

    local = ADAPTER_COUNT // groups
    own_rows = ADAPTER_RANK // owners
    held = sum(partial_sizes)
    padded = -(-held // (8 * 128)) * 8 * 128
    tall = jnp.pad(partial_all, ((0, 0), (0, padded - held)))
    tall = tall.reshape(8 * ADAPTER_RANK, padded // 8)
    scattered = lax.psum_scatter(tall, "expert", scatter_dimension=0, tiled=True)
    scattered = scattered.reshape(own_rows, padded)
    moved = lax.all_to_all(owned_all, "expert", split_axis=0, concat_axis=1, tiled=True)
    joined = jnp.concatenate([scattered, moved], axis=1)
    gathered = lax.all_gather(joined, "dp", axis=0)
    sums = []
    for which in range(local):
        mine = (adapter_groups == group_index * local + which).astype(jnp.float32)
        sums.append(jnp.sum(jnp.where(mine[:, None, None] > 0, gathered, 0.0), axis=0))
    sums = jnp.stack(sums)
    arrived = []
    for step in range(local):
        piece = lax.dynamic_index_in_dim(sums, (step + owner_index) % local, 0, False)
        arrived.append(
            lax.ppermute(
                piece,
                "expert",
                [
                    (source, (step + source) % local * (owners // local) + source // local)
                    for source in range(owners)
                ],
            )
        )
    arrived = jnp.stack(arrived)
    place = owner_index // (owners // local)
    rows = jnp.concatenate(
        [
            lax.dynamic_index_in_dim(arrived, (place - which) % local, 0, False)
            for which in range(local)
        ],
        axis=0,
    )
    pieces = cut(rows[:, :held], partial_sizes)
    wide = rows[:, padded:].reshape(local * own_rows, owners, sum(owned_sizes))
    owned_pieces = [
        value.reshape(local * own_rows, owners * size)
        for value, size in zip(cut(wide, owned_sizes), owned_sizes)
    ]
    return pieces, owned_pieces


def on_device(
    tokens,
    cotangent,
    attention_norm_gain,
    experts_norm_gain,
    attention_query_key_value,
    attention_output_weight,
    router_projection,
    shared_gate_up_weight,
    shared_down_weight,
    shared_gate_vector,
    expert_gate_up_weight,
    expert_down_weight,
    routes,
    lengths,
    adapter_slot_index,
    attention_adapter_first,
    attention_adapter_second,
    router_adapter_first,
    router_adapter_second,
    shared_adapter_first,
    shared_adapter_second,
    shared_down_adapter_first,
    shared_down_adapter_second,
    expert_adapter_first,
    expert_adapter_second,
    expert_down_adapter_first,
    expert_down_adapter_second,
):
    count_rows, model_width_size = tokens.shape
    owners = lax.axis_size("expert")
    owner_index = lax.axis_index("expert")
    experts = router_projection.shape[1]
    top_count = routes.shape[1]
    capacity = (count_rows * top_count * 9 + 8 * experts - 1) // (8 * experts)
    group_rows = count_rows * owners
    seq_length = min(SEQ_MAX, group_rows)
    slot_count = lengths.shape[0]
    group_devices = owners // slot_count
    head_count = HEADS // group_devices
    width = head_count * HEAD_DIM
    own_slot = owner_index // group_devices
    head_start = owner_index % group_devices * head_count
    head_column = head_start * HEAD_DIM
    score_scale = 1.0 / math.sqrt(HEAD_DIM)
    half = jnp.bfloat16

    def own_rows(values):
        return lax.dynamic_slice_in_dim(values, owner_index * count_rows, count_rows, 0)

    def slot_rows(values):
        if slot_count == 1:
            return values
        return lax.dynamic_slice_in_dim(values, own_slot * seq_length, seq_length, 0)

    def group_wide(values):
        if slot_count == 1:
            return values
        return lax.dynamic_update_slice_in_dim(
            jnp.zeros((group_rows, values.shape[1]), values.dtype), values, own_slot * seq_length, 0
        )

    def slot_wide(values):
        if slot_count == 1:
            return values
        return lax.dynamic_update_slice_in_dim(
            jnp.zeros((slot_count * ADAPTER_RANK, values.shape[1]), values.dtype),
            values,
            own_slot * ADAPTER_RANK,
            0,
        )

    def slot_value(values):
        return values[0] if slot_count == 1 else lax.dynamic_index_in_dim(values, own_slot, 0, False)

    def picked_maps(maps, axis):
        return jnp.concatenate(
            [
                lax.dynamic_slice_in_dim(
                    maps, adapter_slot_index[slot] * ADAPTER_RANK, ADAPTER_RANK, axis
                )
                for slot in range(slot_count)
            ],
            axis=axis,
        )

    def scatter_rows(values):
        return lax.psum_scatter(values.astype(half), "expert", scatter_dimension=0, tiled=True)

    tokens_all = lax.all_gather(tokens, "expert", axis=0, tiled=True)
    qkv_weights = head_weights(
        attention_query_key_value, owner_index, owners, slot_count, head_start, width
    )
    routes_all = lax.all_gather(routes, "expert", axis=0, tiled=True)
    adapter_groups = lax.all_gather(adapter_slot_index, "dp", axis=0, tiled=True)
    upstream_all = lax.all_gather(cotangent, "expert", axis=0, tiled=True)
    if attention_output_weight.shape[0] == width:
        output_weight = attention_output_weight
    else:
        output_weight = lax.dynamic_slice_in_dim(
            lax.all_gather(attention_output_weight, "expert", axis=0, tiled=True),
            head_column,
            width,
            0,
        )

    if slot_count == 1:
        selector = None
    else:
        row_slot = jnp.arange(group_rows, dtype=jnp.int32) // seq_length
        rank_slot = jnp.arange(slot_count * ADAPTER_RANK, dtype=jnp.int32) // ADAPTER_RANK
        selector = (row_slot[:, None] == rank_slot[None, :]).astype(half)

    def chosen(values, picker):
        narrow = values.astype(half)
        return narrow if picker is None else narrow * picker

    attention_adapter = slot_value(adapter_slot_index) * ADAPTER_RANK
    attention_first = lax.dynamic_slice_in_dim(
        attention_adapter_first, attention_adapter, ADAPTER_RANK, 2
    )
    attention_second = lax.dynamic_slice_in_dim(
        attention_adapter_second, attention_adapter, ADAPTER_RANK, 1
    )
    qkv_second = lax.dynamic_slice_in_dim(attention_second[:3], head_column, width, 2)
    output_first = lax.dynamic_slice_in_dim(attention_first[3], head_column, width, 0)
    output_second = attention_second[3]
    router_first = picked_maps(router_adapter_first, 1)
    router_second = picked_maps(router_adapter_second, 0)
    shared_wide = shared_down_weight.shape[0]
    shared_first = picked_maps(shared_adapter_first, 2)
    shared_second = lax.dynamic_slice_in_dim(
        picked_maps(shared_adapter_second, 1), owner_index * shared_wide, shared_wide, 2
    )
    down_first = lax.dynamic_slice_in_dim(
        picked_maps(shared_down_adapter_first, 1), owner_index * shared_wide, shared_wide, 0
    )
    down_second = picked_maps(shared_down_adapter_second, 0)
    expert_first = picked_maps(expert_adapter_first[0], 2)
    expert_second = picked_maps(expert_adapter_second[0], 1)
    expert_down_first = picked_maps(expert_down_adapter_first[0], 1)
    expert_down_second = picked_maps(expert_down_adapter_second[0], 0)

    expert_range = jnp.arange(experts, dtype=jnp.int32)
    route_hits = jnp.any(routes_all[:, :, None] == expert_range[None, None, :], axis=1)
    own_hits = jnp.any(routes_all == owner_index, axis=1)
    ranks = jnp.cumsum(own_hits.astype(jnp.int32)) - 1
    row_range = jnp.arange(experts * capacity, dtype=jnp.int32)
    placed = (ranks[None, :] == row_range[:, None]) & own_hits[None, :]
    spread = placed.astype(half)
    row_selector = None if selector is None else narrow_product(spread, selector).astype(half)

    slot_tokens = slot_rows(tokens_all).astype(jnp.float32)
    normed_first, unused = rms_forward(slot_tokens, attention_norm_gain)
    first_narrow = normed_first.astype(half)
    positions = jnp.arange(seq_length, dtype=jnp.int32)
    cosine_table, sine_table = rope_tables(positions, HEAD_DIM)
    shaped = (seq_length, head_count, HEAD_DIM)
    attention_middle = [
        narrow_product(first_narrow, attention_first[kind]).astype(half) for kind in range(3)
    ]
    projected = [
        narrow_product(first_narrow, qkv_weights[kind])
        + narrow_product(attention_middle[kind], qkv_second[kind])
        for kind in range(3)
    ]
    query_low = rotate(projected[0].reshape(shaped), cosine_table, sine_table, 1.0).astype(half)
    key_low = rotate(projected[1].reshape(shaped), cosine_table, sine_table, 1.0).astype(half)
    value_low = projected[2].reshape(shaped).astype(half)
    allowed = ((positions // BLOCK)[None, :] <= (positions // BLOCK)[:, None]) & (
        positions < slot_value(lengths)
    )[None, :]
    scores = (
        jnp.einsum("qhd,khd->hqk", query_low, key_low, preferred_element_type=jnp.float32)
        * score_scale
    )
    scores = jnp.where(allowed[None], scores, MASKED)
    exponents = jnp.exp(scores - jnp.max(scores, axis=2, keepdims=True)) * allowed[None]
    probabilities = exponents / jnp.sum(exponents, axis=2, keepdims=True)
    probabilities_low = probabilities.astype(half)
    attended = jnp.einsum(
        "hqk,khd->qhd", probabilities_low, value_low, preferred_element_type=jnp.float32
    )
    attended_low = attended.reshape(seq_length, width).astype(half)
    output_middle = narrow_product(attended_low, output_first).astype(half)
    attention_part = narrow_product(attended_low, output_weight) + narrow_product(
        output_middle, output_second
    )
    input_rows = tokens.astype(jnp.float32)
    residual_stream = input_rows + scatter_rows(group_wide(attention_part)).astype(jnp.float32)
    normed_second, factor_second = rms_forward(residual_stream, experts_norm_gain)
    second_own = normed_second.astype(half)
    second_all = lax.all_gather(second_own, "expert", axis=0, tiled=True)

    router_middle = chosen(narrow_product(second_all, router_first), selector)
    router_scores = narrow_product(second_all, router_projection) + narrow_product(
        router_middle, router_second
    )
    reach = jnp.max(jnp.where(route_hits, router_scores, MASKED), axis=1, keepdims=True)
    gate_exponents = jnp.where(route_hits, jnp.exp(jnp.minimum(router_scores - reach, 0.0)), 0.0)
    gate_weights = gate_exponents / jnp.sum(gate_exponents, axis=1, keepdims=True)
    own_gate = jnp.sum(jnp.where(expert_range[None, :] == owner_index, gate_weights, 0.0), axis=1)
    row_gate = jnp.sum(jnp.where(placed, own_gate[None, :], 0.0), axis=1, keepdims=True)
    shared_weight = jax.nn.sigmoid(
        narrow_product(second_all, shared_gate_vector[:, None])
    )

    expert_rows = narrow_product(spread, second_all).astype(half)
    expert_middle = [
        chosen(narrow_product(expert_rows, expert_first[kind]), row_selector) for kind in range(2)
    ]
    expert_pre = [
        narrow_product(expert_rows, expert_gate_up_weight[0, kind])
        + narrow_product(expert_middle[kind], expert_second[kind])
        for kind in range(2)
    ]
    expert_hidden = (jax.nn.silu(expert_pre[0]) * expert_pre[1]).astype(half)
    expert_down_middle = chosen(narrow_product(expert_hidden, expert_down_first), row_selector)
    expert_result = (
        narrow_product(expert_hidden, expert_down_weight[0])
        + narrow_product(expert_down_middle, expert_down_second)
    ).astype(half)

    shared_middle = [
        chosen(narrow_product(second_all, shared_first[kind]), selector) for kind in range(2)
    ]
    shared_pre = [
        narrow_product(second_all, shared_gate_up_weight[kind])
        + narrow_product(shared_middle[kind], shared_second[kind])
        for kind in range(2)
    ]
    shared_hidden = (jax.nn.silu(shared_pre[0]) * shared_pre[1]).astype(half)
    down_middle = chosen(narrow_product(shared_hidden, down_first), selector)
    shared_part = narrow_product(shared_hidden, shared_down_weight) + narrow_product(
        down_middle, down_second
    )
    upstream_wide = upstream_all.astype(jnp.float32)
    shared_dot = jnp.sum(upstream_wide * shared_part, axis=1)

    upstream_rows = narrow_product(spread, upstream_all)
    row_dot = jnp.sum(upstream_rows * expert_result.astype(jnp.float32), axis=1, keepdims=True)
    gate_dot = jnp.sum(jnp.where(placed, row_dot, 0.0), axis=0)
    expert_upstream = (row_gate * upstream_rows).astype(half)
    expert_down_inner = chosen(rows_product(expert_upstream, expert_down_second), row_selector)
    expert_grad_hidden = rows_product(expert_upstream, expert_down_weight[0]) + rows_product(
        expert_down_inner, expert_down_first
    )
    expert_grad_pre = gated_back(expert_pre[0], expert_pre[1], expert_grad_hidden)
    expert_inner = [
        chosen(rows_product(expert_grad_pre[kind], expert_second[kind]), row_selector)
        for kind in range(2)
    ]
    copy_grad = sum(
        rows_product(expert_grad_pre[kind], expert_gate_up_weight[0, kind])
        + rows_product(expert_inner[kind], expert_first[kind])
        for kind in range(2)
    ).astype(half)

    value_grads = (shared_weight * upstream_wide).astype(half)
    down_inner = chosen(rows_product(value_grads, down_second), selector)
    shared_grad_hidden = rows_product(value_grads, shared_down_weight) + rows_product(
        down_inner, down_first
    )
    shared_grad_pre = gated_back(shared_pre[0], shared_pre[1], shared_grad_hidden)
    shared_inner = [
        chosen(rows_product(shared_grad_pre[kind], shared_second[kind]), selector)
        for kind in range(2)
    ]
    second_part = token_product(spread, copy_grad) + sum(
        rows_product(shared_grad_pre[kind], shared_gate_up_weight[kind])
        + rows_product(shared_inner[kind], shared_first[kind])
        for kind in range(2)
    )
    dots = jnp.concatenate(
        [
            jnp.where(expert_range[:, None] == owner_index, gate_dot[None, :], 0.0),
            shared_dot[None, :],
            jnp.zeros((7, group_rows), jnp.float32),
        ],
        axis=0,
    )
    own_dots = jnp.transpose(lax.psum_scatter(dots, "expert", scatter_dimension=1, tiled=True))
    second_sum = scatter_rows(second_part).astype(jnp.float32)
    layer_part = (
        token_product(spread, (row_gate * expert_result.astype(jnp.float32)).astype(half))
        + shared_weight * shared_part
    )

    own_weights = own_rows(gate_weights)
    gate_grads = own_dots[:, :experts]
    centered = own_weights * (
        gate_grads - jnp.sum(own_weights * gate_grads, axis=1, keepdims=True)
    )
    logit_grads = centered.astype(half)
    own_selector = None if selector is None else own_rows(selector)
    router_inner = chosen(rows_product(logit_grads, router_second), own_selector)
    own_shared_weight = own_rows(shared_weight)
    weight_grads = own_dots[:, experts : experts + 1] * own_shared_weight * (1.0 - own_shared_weight)
    second_grad = (
        second_sum
        + rows_product(logit_grads, router_projection)
        + rows_product(router_inner, router_first)
        + weight_grads * shared_gate_vector.astype(jnp.float32)[None, :]
    )
    residual_grad = cotangent.astype(jnp.float32) + rms_backward(
        residual_stream, factor_second, experts_norm_gain, second_grad
    )
    output_upstream = slot_rows(
        lax.all_gather(residual_grad.astype(half), "expert", axis=0, tiled=True)
    )

    output_inner = rows_product(output_upstream, output_second).astype(half)
    attended_grad = (
        (rows_product(output_upstream, output_weight) + rows_product(output_inner, output_first))
        .astype(half)
        .reshape(shaped)
    )
    row_delta = jnp.transpose(jnp.sum(attended_grad.astype(jnp.float32) * attended, axis=2))
    prob_grads = jnp.einsum(
        "qhd,khd->hqk", attended_grad, value_low, preferred_element_type=jnp.float32
    )
    score_grad = (probabilities * (prob_grads - row_delta[:, :, None])).astype(half)
    query_grad = (
        jnp.einsum("hqk,khd->qhd", score_grad, key_low, preferred_element_type=jnp.float32)
        * score_scale
    )
    key_grad = (
        jnp.einsum("hqk,qhd->khd", score_grad, query_low, preferred_element_type=jnp.float32)
        * score_scale
    )
    value_grad = jnp.einsum(
        "hqk,qhd->khd", probabilities_low, attended_grad, preferred_element_type=jnp.float32
    )
    pre_grads = [
        rotate(query_grad, cosine_table, sine_table, -1.0).astype(half).reshape(seq_length, width),
        rotate(key_grad, cosine_table, sine_table, -1.0).astype(half).reshape(seq_length, width),
        value_grad.astype(half).reshape(seq_length, width),
    ]
    qkv_inner = [rows_product(pre_grads[kind], qkv_second[kind]).astype(half) for kind in range(3)]
    first_part = sum(
        rows_product(pre_grads[kind], qkv_weights[kind])
        + rows_product(qkv_inner[kind], attention_first[kind])
        for kind in range(3)
    )
    first_grad = scatter_rows(group_wide(first_part)).astype(jnp.float32)
    unused, factor_first = rms_forward(input_rows, attention_norm_gain)
    tokens_grad = residual_grad + rms_backward(
        input_rows, factor_first, attention_norm_gain, first_grad
    )
    layer_out = (residual_stream + scatter_rows(layer_part).astype(jnp.float32)).astype(half)

    own_router_middle = own_rows(router_middle)
    early, early_own = reduce_adapters(
        [
            slot_wide(token_product(output_middle, output_upstream)),
            token_product(shared_inner[0], second_all),
            token_product(shared_inner[1], second_all),
            token_product(down_middle, value_grads),
            token_product(router_inner, second_own),
            token_product(own_router_middle, logit_grads),
        ],
        [
            slot_wide(token_product(output_inner, attended_low)),
            token_product(shared_middle[0], shared_grad_pre[0]),
            token_product(shared_middle[1], shared_grad_pre[1]),
            token_product(down_inner, shared_hidden),
        ],
        [head_column] + [owner_index * shared_wide] * 3,
        [model_width_size] + [owners * shared_wide] * 3,
        adapter_slot_index,
        adapter_groups,
        owner_index,
        owners,
    )
    late, late_own = reduce_adapters(
        [slot_wide(token_product(qkv_inner[kind], first_narrow)) for kind in range(3)],
        [slot_wide(token_product(attention_middle[kind], pre_grads[kind])) for kind in range(3)],
        [head_column] * 3,
        [model_width_size] * 3,
        adapter_slot_index,
        adapter_groups,
        owner_index,
        owners,
    )
    attn_grad_a = jnp.stack([jnp.transpose(value) for value in late + [early_own[0]]])
    attn_grad_b = jnp.stack(late_own + [early[0]])

    wide_grads = jnp.concatenate(
        [
            token_product(expert_inner[0], expert_rows),
            token_product(expert_inner[1], expert_rows),
            token_product(expert_middle[0], expert_grad_pre[0]),
            token_product(expert_middle[1], expert_grad_pre[1]),
            token_product(expert_down_inner, expert_hidden),
            token_product(expert_down_middle, expert_upstream),
        ],
        axis=1,
    ).astype(half)
    expert_grads = lax.all_gather(wide_grads, "dp", axis=0, tiled=True)
    rank_range = jnp.arange(ADAPTER_COUNT * ADAPTER_RANK, dtype=jnp.int32)
    source_rank = jnp.arange(expert_grads.shape[0], dtype=jnp.int32)
    source_place = jnp.repeat(adapter_groups, ADAPTER_RANK) * ADAPTER_RANK + (
        source_rank % ADAPTER_RANK
    )
    placement = (source_place[:, None] == rank_range[None, :]).astype(half)
    feed = expert_down_weight.shape[1]
    bounds = [0, model_width_size, 2 * model_width_size]
    bounds += [bounds[-1] + feed, bounds[-1] + 2 * feed, bounds[-1] + 3 * feed]
    expert_pieces = [
        expert_grads[:, start:stop] for start, stop in zip(bounds, bounds[1:] + [None])
    ]
    in_grad_a = jnp.stack([token_product(value, placement) for value in expert_pieces[:2]])
    in_grad_b = jnp.stack([token_product(placement, value) for value in expert_pieces[2:4]])
    down_grad_a = token_product(expert_pieces[4], placement)
    down_grad_b = token_product(placement, expert_pieces[5])
    return (
        layer_out,
        tokens_grad,
        attn_grad_a,
        attn_grad_b,
        jnp.transpose(early[4]),
        early[5],
        jnp.stack([jnp.transpose(early[1]), jnp.transpose(early[2])]),
        jnp.stack(early_own[1:3]),
        jnp.transpose(early_own[3]),
        early[3],
        in_grad_a[None],
        in_grad_b[None],
        down_grad_a[None],
        down_grad_b[None],
    )


def solution(mesh):
    return jax.shard_map(
        on_device,
        mesh=mesh,
        in_specs=(
            P(("dp", "expert"), None),
            P(("dp", "expert"), None),
            P(),
            P(),
            P(None, "expert"),
            P("expert", None),
            P(),
            P(None, None, "expert"),
            P("expert", None),
            P(),
            P("expert", None, None, None),
            P("expert", None, None),
            P(("dp", "expert"), None),
            P("dp"),
            P("dp"),
            P(),
            P(),
            P(),
            P(),
            P(),
            P(),
            P(),
            P(),
            P("expert", None, None, None),
            P("expert", None, None, None),
            P("expert", None, None),
            P("expert", None, None),
        ),
        out_specs=(
            P(("dp", "expert"), None),
            P(("dp", "expert"), None),
            P(None, None, ("dp", "expert")),
            P(None, ("dp", "expert"), None),
            P(None, ("dp", "expert")),
            P(("dp", "expert"), None),
            P(None, None, ("dp", "expert")),
            P(None, ("dp", "expert"), None),
            P(None, ("dp", "expert")),
            P(("dp", "expert"), None),
            P("expert", None, None, None),
            P("expert", None, None, None),
            P("expert", None, None),
            P("expert", None, None),
        ),
        check_vma=False,
    )
```

```python
import math

import jax
import jax.numpy as jnp
from jax import lax
from jax.sharding import PartitionSpec as P

HEADS = 16
HEAD_DIM = 128
ADAPTER_RANK = 16
ADAPTER_COUNT = 8
BLOCK = 256
SEQ_MAX = 2048


NORM_EPS = 1e-06
ROPE_BASE = 1000000.0
MASKED = -1e30


def narrow_product(left_side, right_side):
    return jnp.dot(left_side, right_side, preferred_element_type=jnp.float32)


def rms_forward(values, gain_vector):
    factor = lax.rsqrt(jnp.mean(values * values, axis=-1, keepdims=True) + NORM_EPS)
    return (values * factor * gain_vector, factor)


def rms_backward(values, factor, gain_vector, upstream):
    weighted = upstream * gain_vector
    return factor * weighted - values * (factor * factor * factor) * jnp.mean(
        values * weighted, axis=-1, keepdims=True
    )


def rope_tables(positions, head_width):
    half_width = head_width // 2
    inverse = ROPE_BASE ** (-(jnp.arange(half_width).astype(jnp.float32) * 2.0 / head_width))
    angles = positions.astype(jnp.float32)[:, None] * inverse[None, :]
    return (jnp.cos(angles), jnp.sin(angles))


def rotate(values, cosine_table, sine_table, direction):
    half_width = values.shape[-1] // 2
    first_half = values[..., :half_width]
    second_half = values[..., half_width:]
    cosine_part = cosine_table[:, None, :]
    sine_part = sine_table[:, None, :] * direction
    return jnp.concatenate(
        [
            first_half * cosine_part - second_half * sine_part,
            second_half * cosine_part + first_half * sine_part,
        ],
        axis=-1,
    )


def rows_product(left_side, right_side):
    return lax.dot_general(
        left_side, right_side, (((1,), (1,)), ((), ())), preferred_element_type=jnp.float32
    )


def token_product(left_side, right_side):
    return lax.dot_general(
        left_side, right_side, (((0,), (0,)), ((), ())), preferred_element_type=jnp.float32
    )


def gated_back(gate_value, up_value, grad_hidden):
    sigmoid_gate = jax.nn.sigmoid(gate_value)
    grad_gate = grad_hidden * up_value * sigmoid_gate * (1.0 + gate_value * (1.0 - sigmoid_gate))
    grad_up = grad_hidden * gate_value * sigmoid_gate
    return (grad_gate.astype(jnp.bfloat16), grad_up.astype(jnp.bfloat16))


def head_weights(columns, owner_index, owners, slot_count, head_start, width):
    model_width_size, held = columns.shape
    groups = lax.axis_size("dp")
    group_index = lax.axis_index("dp")
    if slot_count == 1 and held == 3 * width and owners % 3 and groups & (groups - 1) == 0:
        share = model_width_size // groups
        mine = lax.dynamic_slice_in_dim(columns, group_index * share, share, 0)
        moved = jnp.stack(
            [
                lax.ppermute(
                    mine[:, step * width : (step + 1) * width],
                    "expert",
                    [(source, (3 * source + step) % owners) for source in range(owners)],
                )
                for step in range(3)
            ]
        )
        kinds = jnp.stack(
            [
                lax.dynamic_index_in_dim(moved, (owner_index + owners * kind) % 3, 0, False)
                for kind in range(3)
            ]
        )
        shares = jnp.stack(
            [kinds]
            + [
                lax.ppermute(kinds, "dp", [(source, source ^ step) for source in range(groups)])
                for step in range(1, groups)
            ]
        )
        return jnp.concatenate(
            [
                lax.dynamic_index_in_dim(shares, group_index ^ place, 0, False)
                for place in range(groups)
            ],
            axis=1,
        )
    full = lax.all_gather(columns, "expert", axis=1, tiled=True)
    return jnp.stack(
        [
            lax.dynamic_slice_in_dim(full, kind * model_width_size + head_start * HEAD_DIM, width, 1)
            for kind in range(3)
        ]
    )


def spread_adapters(compact, adapter_index):
    ranks = ADAPTER_COUNT * ADAPTER_RANK
    total = jnp.zeros((ranks, compact.shape[1]), compact.dtype)
    for slot in range(adapter_index.shape[0]):
        piece = compact[slot * ADAPTER_RANK : (slot + 1) * ADAPTER_RANK]
        total = total + lax.dynamic_update_slice_in_dim(
            jnp.zeros_like(total), piece, adapter_index[slot] * ADAPTER_RANK, 0
        )
    return total


def reduce_adapters(
    partial, owned, owned_starts, owned_totals, adapter_index, owner_index, owners
):
    groups = lax.axis_size("dp")
    group_index = lax.axis_index("dp")
    slot_count = adapter_index.shape[0]
    partial_sizes = [value.shape[1] for value in partial]
    owned_sizes = [value.shape[1] for value in owned]
    partial_all = jnp.concatenate(partial, axis=1)
    owned_all = jnp.concatenate(owned, axis=1)

    def cut(values, sizes):
        pieces, at = [], 0
        for size in sizes:
            pieces.append(values[..., at : at + size])
            at += size
        return pieces

    if slot_count > 1 or ADAPTER_RANK % owners or ADAPTER_COUNT % groups or owners % (
        ADAPTER_COUNT // groups
    ):
        wide = [
            lax.dynamic_update_slice_in_dim(
                jnp.zeros((value.shape[0], total), value.dtype), value, start, 1
            )
            for value, start, total in zip(owned, owned_starts, owned_totals)
        ]
        dense = spread_adapters(jnp.concatenate([partial_all] + wide, axis=1), adapter_index)
        summed = lax.psum_scatter(dense, ("dp", "expert"), scatter_dimension=0, tiled=True)
        pieces = cut(summed, partial_sizes + owned_totals)
        return pieces[: len(partial)], pieces[len(partial) :]

    local = ADAPTER_COUNT // groups
    own_rows = ADAPTER_RANK // owners
    held = sum(partial_sizes)
    joined = jnp.concatenate([partial_all, owned_all], axis=1).astype(jnp.bfloat16)
    moved = lax.all_to_all(
        joined.reshape(owners, own_rows, joined.shape[1]),
        "expert",
        split_axis=0,
        concat_axis=0,
        tiled=True,
    )
    scattered = jnp.sum(moved[:, :, :held].astype(jnp.float32), axis=0).astype(jnp.bfloat16)
    placed = [
        jnp.transpose(value, (1, 0, 2)).reshape(own_rows, owners * size)
        for value, size in zip(cut(moved[:, :, held:], owned_sizes), owned_sizes)
    ]
    label = jnp.broadcast_to(adapter_index[:, None], (own_rows, 128)).astype(jnp.bfloat16)
    gathered = lax.all_gather(
        jnp.concatenate([scattered] + placed + [label], axis=1), "dp", axis=0
    ).astype(jnp.float32)
    labels = gathered[:, :, -1:]
    gathered = gathered[:, :, :-128]
    sums = []
    for which in range(local):
        wanted = labels == (group_index * local + which).astype(jnp.float32)
        sums.append(jnp.sum(jnp.where(wanted, gathered, 0.0), axis=0))
    sums = jnp.stack(sums).astype(jnp.bfloat16)
    arrived = []
    for step in range(local):
        piece = lax.dynamic_index_in_dim(sums, (step + owner_index) % local, 0, False)
        arrived.append(
            lax.ppermute(
                piece,
                "expert",
                [
                    (source, (step + source) % local * (owners // local) + source // local)
                    for source in range(owners)
                ],
            )
        )
    arrived = jnp.stack(arrived)
    place = owner_index // (owners // local)
    rows = jnp.concatenate(
        [
            lax.dynamic_index_in_dim(arrived, (place - which) % local, 0, False)
            for which in range(local)
        ],
        axis=0,
    )
    pieces = cut(rows.astype(jnp.float32), partial_sizes + [owners * size for size in owned_sizes])
    return pieces[: len(partial)], pieces[len(partial) :]


def on_device(
    tokens,
    cotangent,
    attention_norm_gain,
    experts_norm_gain,
    attention_query_key_value,
    attention_output_weight,
    router_projection,
    shared_gate_up_weight,
    shared_down_weight,
    shared_gate_vector,
    expert_gate_up_weight,
    expert_down_weight,
    routes,
    lengths,
    adapter_slot_index,
    attention_adapter_first,
    attention_adapter_second,
    router_adapter_first,
    router_adapter_second,
    shared_adapter_first,
    shared_adapter_second,
    shared_down_adapter_first,
    shared_down_adapter_second,
    expert_adapter_first,
    expert_adapter_second,
    expert_down_adapter_first,
    expert_down_adapter_second,
):
    count_rows, model_width_size = tokens.shape
    owners = lax.axis_size("expert")
    owner_index = lax.axis_index("expert")
    experts = router_projection.shape[1]
    top_count = routes.shape[1]
    capacity = (count_rows * top_count * 9 + 8 * experts - 1) // (8 * experts)
    group_rows = count_rows * owners
    seq_length = min(SEQ_MAX, group_rows)
    slot_count = lengths.shape[0]
    group_devices = owners // slot_count
    head_count = HEADS // group_devices
    width = head_count * HEAD_DIM
    own_slot = owner_index // group_devices
    head_start = owner_index % group_devices * head_count
    head_column = head_start * HEAD_DIM
    score_scale = 1.0 / math.sqrt(HEAD_DIM)
    half = jnp.bfloat16

    def own_rows(values):
        return lax.dynamic_slice_in_dim(values, owner_index * count_rows, count_rows, 0)

    def slot_rows(values):
        if slot_count == 1:
            return values
        return lax.dynamic_slice_in_dim(values, own_slot * seq_length, seq_length, 0)

    def group_wide(values):
        if slot_count == 1:
            return values
        return lax.dynamic_update_slice_in_dim(
            jnp.zeros((group_rows, values.shape[1]), values.dtype), values, own_slot * seq_length, 0
        )

    def slot_wide(values):
        if slot_count == 1:
            return values
        return lax.dynamic_update_slice_in_dim(
            jnp.zeros((slot_count * ADAPTER_RANK, values.shape[1]), values.dtype),
            values,
            own_slot * ADAPTER_RANK,
            0,
        )

    def slot_value(values):
        return values[0] if slot_count == 1 else lax.dynamic_index_in_dim(values, own_slot, 0, False)

    def picked_maps(maps, axis):
        return jnp.concatenate(
            [
                lax.dynamic_slice_in_dim(
                    maps, adapter_slot_index[slot] * ADAPTER_RANK, ADAPTER_RANK, axis
                )
                for slot in range(slot_count)
            ],
            axis=axis,
        )

    def scatter_rows(values):
        return lax.psum_scatter(values.astype(half), "expert", scatter_dimension=0, tiled=True)

    tokens_all = lax.all_gather(tokens, "expert", axis=0, tiled=True)
    qkv_weights = head_weights(
        attention_query_key_value, owner_index, owners, slot_count, head_start, width
    )
    routes_all = lax.all_gather(routes, "expert", axis=0, tiled=True)
    tokens_all, routes_all = lax.optimization_barrier((tokens_all, routes_all))
    upstream_all = lax.all_gather(cotangent, "expert", axis=0, tiled=True)
    if attention_output_weight.shape[0] == width:
        output_weight = attention_output_weight
    else:
        output_weight = lax.dynamic_slice_in_dim(
            lax.all_gather(attention_output_weight, "expert", axis=0, tiled=True),
            head_column,
            width,
            0,
        )

    if slot_count == 1:
        selector = None
    else:
        row_slot = jnp.arange(group_rows, dtype=jnp.int32) // seq_length
        rank_slot = jnp.arange(slot_count * ADAPTER_RANK, dtype=jnp.int32) // ADAPTER_RANK
        selector = (row_slot[:, None] == rank_slot[None, :]).astype(half)

    def chosen(values, picker):
        narrow = values.astype(half)
        return narrow if picker is None else narrow * picker

    attention_adapter = slot_value(adapter_slot_index) * ADAPTER_RANK
    attention_first = lax.dynamic_slice_in_dim(
        attention_adapter_first, attention_adapter, ADAPTER_RANK, 2
    )
    attention_second = lax.dynamic_slice_in_dim(
        attention_adapter_second, attention_adapter, ADAPTER_RANK, 1
    )
    qkv_second = lax.dynamic_slice_in_dim(attention_second[:3], head_column, width, 2)
    output_first = lax.dynamic_slice_in_dim(attention_first[3], head_column, width, 0)
    output_second = attention_second[3]
    router_first = picked_maps(router_adapter_first, 1)
    router_second = picked_maps(router_adapter_second, 0)
    shared_wide = shared_down_weight.shape[0]
    shared_first = picked_maps(shared_adapter_first, 2)
    shared_second = lax.dynamic_slice_in_dim(
        picked_maps(shared_adapter_second, 1), owner_index * shared_wide, shared_wide, 2
    )
    down_first = lax.dynamic_slice_in_dim(
        picked_maps(shared_down_adapter_first, 1), owner_index * shared_wide, shared_wide, 0
    )
    down_second = picked_maps(shared_down_adapter_second, 0)
    expert_first = picked_maps(expert_adapter_first[0], 2)
    expert_second = picked_maps(expert_adapter_second[0], 1)
    expert_down_first = picked_maps(expert_down_adapter_first[0], 1)
    expert_down_second = picked_maps(expert_down_adapter_second[0], 0)

    expert_range = jnp.arange(experts, dtype=jnp.int32)
    route_hits = jnp.any(routes_all[:, :, None] == expert_range[None, None, :], axis=1)
    own_hits = jnp.any(routes_all == owner_index, axis=1)
    ranks = jnp.cumsum(own_hits.astype(jnp.int32)) - 1
    row_range = jnp.arange(experts * capacity, dtype=jnp.int32)
    placed = (ranks[None, :] == row_range[:, None]) & own_hits[None, :]
    spread = placed.astype(half)
    row_selector = None if selector is None else narrow_product(spread, selector).astype(half)

    slot_tokens = slot_rows(tokens_all).astype(jnp.float32)
    normed_first, unused = rms_forward(slot_tokens, attention_norm_gain)
    first_narrow = normed_first.astype(half)
    positions = jnp.arange(seq_length, dtype=jnp.int32)
    cosine_table, sine_table = rope_tables(positions, HEAD_DIM)
    shaped = (seq_length, head_count, HEAD_DIM)
    attention_middle = [
        narrow_product(first_narrow, attention_first[kind]).astype(half) for kind in range(3)
    ]
    projected = [
        narrow_product(first_narrow, qkv_weights[kind])
        + narrow_product(attention_middle[kind], qkv_second[kind])
        for kind in range(3)
    ]
    query_low = rotate(projected[0].reshape(shaped), cosine_table, sine_table, 1.0).astype(half)
    key_low = rotate(projected[1].reshape(shaped), cosine_table, sine_table, 1.0).astype(half)
    value_low = projected[2].reshape(shaped).astype(half)
    allowed = ((positions // BLOCK)[None, :] <= (positions // BLOCK)[:, None]) & (
        positions < slot_value(lengths)
    )[None, :]
    scores = (
        jnp.einsum("qhd,khd->hqk", query_low, key_low, preferred_element_type=jnp.float32)
        * score_scale
    )
    scores = jnp.where(allowed[None], scores, MASKED)
    exponents = jnp.exp(scores - jnp.max(scores, axis=2, keepdims=True)) * allowed[None]
    probabilities = exponents / jnp.sum(exponents, axis=2, keepdims=True)
    probabilities_low = probabilities.astype(half)
    attended = jnp.einsum(
        "hqk,khd->qhd", probabilities_low, value_low, preferred_element_type=jnp.float32
    )
    attended_low = attended.reshape(seq_length, width).astype(half)
    output_middle = narrow_product(attended_low, output_first).astype(half)
    attention_part = narrow_product(attended_low, output_weight) + narrow_product(
        output_middle, output_second
    )
    input_rows = tokens.astype(jnp.float32)
    residual_stream = input_rows + scatter_rows(group_wide(attention_part)).astype(jnp.float32)
    normed_second, factor_second = rms_forward(residual_stream, experts_norm_gain)
    second_own = normed_second.astype(half)
    second_all = lax.all_gather(second_own, "expert", axis=0, tiled=True)

    router_middle = chosen(narrow_product(second_all, router_first), selector)
    router_scores = narrow_product(second_all, router_projection) + narrow_product(
        router_middle, router_second
    )
    reach = jnp.max(jnp.where(route_hits, router_scores, MASKED), axis=1, keepdims=True)
    gate_exponents = jnp.where(route_hits, jnp.exp(jnp.minimum(router_scores - reach, 0.0)), 0.0)
    gate_weights = gate_exponents / jnp.sum(gate_exponents, axis=1, keepdims=True)
    own_gate = jnp.sum(jnp.where(expert_range[None, :] == owner_index, gate_weights, 0.0), axis=1)
    row_gate = jnp.sum(jnp.where(placed, own_gate[None, :], 0.0), axis=1, keepdims=True)
    shared_weight = jax.nn.sigmoid(
        narrow_product(second_all, shared_gate_vector[:, None])
    )

    expert_rows = narrow_product(spread, second_all).astype(half)
    expert_middle = [
        chosen(narrow_product(expert_rows, expert_first[kind]), row_selector) for kind in range(2)
    ]
    expert_pre = [
        narrow_product(expert_rows, expert_gate_up_weight[0, kind])
        + narrow_product(expert_middle[kind], expert_second[kind])
        for kind in range(2)
    ]
    expert_hidden = (jax.nn.silu(expert_pre[0]) * expert_pre[1]).astype(half)
    expert_down_middle = chosen(narrow_product(expert_hidden, expert_down_first), row_selector)
    expert_result = (
        narrow_product(expert_hidden, expert_down_weight[0])
        + narrow_product(expert_down_middle, expert_down_second)
    ).astype(half)

    shared_middle = [
        chosen(narrow_product(second_all, shared_first[kind]), selector) for kind in range(2)
    ]
    shared_pre = [
        narrow_product(second_all, shared_gate_up_weight[kind])
        + narrow_product(shared_middle[kind], shared_second[kind])
        for kind in range(2)
    ]
    shared_hidden = (jax.nn.silu(shared_pre[0]) * shared_pre[1]).astype(half)
    down_middle = chosen(narrow_product(shared_hidden, down_first), selector)
    shared_part = narrow_product(shared_hidden, shared_down_weight) + narrow_product(
        down_middle, down_second
    )
    layer_part = (
        token_product(spread, (row_gate * expert_result.astype(jnp.float32)).astype(half))
        + shared_weight * shared_part
    )
    layer_sum = scatter_rows(layer_part)
    upstream_wide = upstream_all.astype(jnp.float32)
    shared_dot = jnp.sum(upstream_wide * shared_part, axis=1)

    upstream_rows = narrow_product(spread, upstream_all)
    row_dot = jnp.sum(upstream_rows * expert_result.astype(jnp.float32), axis=1, keepdims=True)
    gate_dot = jnp.sum(jnp.where(placed, row_dot, 0.0), axis=0)
    expert_upstream = (row_gate * upstream_rows).astype(half)
    expert_down_inner = chosen(rows_product(expert_upstream, expert_down_second), row_selector)
    expert_grad_hidden = rows_product(expert_upstream, expert_down_weight[0]) + rows_product(
        expert_down_inner, expert_down_first
    )
    expert_grad_pre = gated_back(expert_pre[0], expert_pre[1], expert_grad_hidden)
    expert_inner = [
        chosen(rows_product(expert_grad_pre[kind], expert_second[kind]), row_selector)
        for kind in range(2)
    ]
    copy_grad = sum(
        rows_product(expert_grad_pre[kind], expert_gate_up_weight[0, kind])
        + rows_product(expert_inner[kind], expert_first[kind])
        for kind in range(2)
    ).astype(half)

    value_grads = (shared_weight * upstream_wide).astype(half)
    down_inner = chosen(rows_product(value_grads, down_second), selector)
    shared_grad_hidden = rows_product(value_grads, shared_down_weight) + rows_product(
        down_inner, down_first
    )
    shared_grad_pre = gated_back(shared_pre[0], shared_pre[1], shared_grad_hidden)
    shared_inner = [
        chosen(rows_product(shared_grad_pre[kind], shared_second[kind]), selector)
        for kind in range(2)
    ]
    copy_grad, layer_sum = lax.optimization_barrier((copy_grad, layer_sum))
    second_part = token_product(spread, copy_grad) + sum(
        rows_product(shared_grad_pre[kind], shared_gate_up_weight[kind])
        + rows_product(shared_inner[kind], shared_first[kind])
        for kind in range(2)
    )
    dots = jnp.concatenate(
        [
            jnp.where(expert_range[:, None] == owner_index, gate_dot[None, :], 0.0),
            shared_dot[None, :],
            jnp.zeros((7, group_rows), jnp.float32),
        ],
        axis=0,
    )
    own_dots = jnp.transpose(lax.psum_scatter(dots, "expert", scatter_dimension=1, tiled=True))
    second_sum = scatter_rows(second_part).astype(jnp.float32)
    own_weights = own_rows(gate_weights)
    gate_grads = own_dots[:, :experts]
    centered = own_weights * (
        gate_grads - jnp.sum(own_weights * gate_grads, axis=1, keepdims=True)
    )
    logit_grads = centered.astype(half)
    own_selector = None if selector is None else own_rows(selector)
    router_inner = chosen(rows_product(logit_grads, router_second), own_selector)
    own_shared_weight = own_rows(shared_weight)
    weight_grads = own_dots[:, experts : experts + 1] * own_shared_weight * (1.0 - own_shared_weight)
    second_grad = (
        second_sum
        + rows_product(logit_grads, router_projection)
        + rows_product(router_inner, router_first)
        + weight_grads * shared_gate_vector.astype(jnp.float32)[None, :]
    )
    residual_grad = cotangent.astype(jnp.float32) + rms_backward(
        residual_stream, factor_second, experts_norm_gain, second_grad
    )
    output_upstream = slot_rows(
        lax.all_gather(residual_grad.astype(half), "expert", axis=0, tiled=True)
    )

    output_inner = rows_product(output_upstream, output_second).astype(half)
    attended_grad = (
        (rows_product(output_upstream, output_weight) + rows_product(output_inner, output_first))
        .astype(half)
        .reshape(shaped)
    )
    row_delta = jnp.transpose(jnp.sum(attended_grad.astype(jnp.float32) * attended, axis=2))
    prob_grads = jnp.einsum(
        "qhd,khd->hqk", attended_grad, value_low, preferred_element_type=jnp.float32
    )
    score_grad = (probabilities * (prob_grads - row_delta[:, :, None])).astype(half)
    query_grad = (
        jnp.einsum("hqk,khd->qhd", score_grad, key_low, preferred_element_type=jnp.float32)
        * score_scale
    )
    key_grad = (
        jnp.einsum("hqk,qhd->khd", score_grad, query_low, preferred_element_type=jnp.float32)
        * score_scale
    )
    value_grad = jnp.einsum(
        "hqk,qhd->khd", probabilities_low, attended_grad, preferred_element_type=jnp.float32
    )
    pre_grads = [
        rotate(query_grad, cosine_table, sine_table, -1.0).astype(half).reshape(seq_length, width),
        rotate(key_grad, cosine_table, sine_table, -1.0).astype(half).reshape(seq_length, width),
        value_grad.astype(half).reshape(seq_length, width),
    ]
    qkv_inner = [rows_product(pre_grads[kind], qkv_second[kind]).astype(half) for kind in range(3)]
    first_part = sum(
        rows_product(pre_grads[kind], qkv_weights[kind])
        + rows_product(qkv_inner[kind], attention_first[kind])
        for kind in range(3)
    )
    first_grad = scatter_rows(group_wide(first_part)).astype(jnp.float32)
    unused, factor_first = rms_forward(input_rows, attention_norm_gain)
    tokens_grad = residual_grad + rms_backward(
        input_rows, factor_first, attention_norm_gain, first_grad
    )
    layer_out = (residual_stream + layer_sum.astype(jnp.float32)).astype(half)

    own_router_middle = own_rows(router_middle)
    router_grad_b = token_product(own_router_middle, logit_grads)
    spare = -experts % 128
    summed, owned = reduce_adapters(
        [slot_wide(token_product(qkv_inner[kind], first_narrow)) for kind in range(3)]
        + [
            slot_wide(token_product(output_middle, output_upstream)),
            token_product(shared_inner[0], second_all),
            token_product(shared_inner[1], second_all),
            token_product(down_middle, value_grads),
            token_product(router_inner, second_own),
            jnp.pad(router_grad_b, ((0, 0), (0, spare))),
        ],
        [slot_wide(token_product(attention_middle[kind], pre_grads[kind])) for kind in range(3)]
        + [
            slot_wide(token_product(output_inner, attended_low)),
            token_product(shared_middle[0], shared_grad_pre[0]),
            token_product(shared_middle[1], shared_grad_pre[1]),
            token_product(down_inner, shared_hidden),
        ],
        [head_column] * 4 + [owner_index * shared_wide] * 3,
        [model_width_size] * 4 + [owners * shared_wide] * 3,
        adapter_slot_index,
        owner_index,
        owners,
    )
    attn_grad_a = jnp.stack([jnp.transpose(value) for value in summed[:3] + owned[3:4]])
    attn_grad_b = jnp.stack(owned[:3] + summed[3:4])

    wide_grads = jnp.concatenate(
        [
            token_product(expert_inner[0], expert_rows),
            token_product(expert_inner[1], expert_rows),
            token_product(expert_middle[0], expert_grad_pre[0]),
            token_product(expert_middle[1], expert_grad_pre[1]),
            token_product(expert_down_inner, expert_hidden),
            token_product(expert_down_middle, expert_upstream),
            jnp.broadcast_to(
                jnp.repeat(adapter_slot_index, ADAPTER_RANK).astype(jnp.float32)[:, None],
                (slot_count * ADAPTER_RANK, 128),
            ),
        ],
        axis=1,
    ).astype(half)
    expert_grads = lax.all_gather(wide_grads, "dp", axis=0, tiled=True)
    rank_range = jnp.arange(ADAPTER_COUNT * ADAPTER_RANK, dtype=jnp.int32)
    source_rank = jnp.arange(expert_grads.shape[0], dtype=jnp.int32)
    source_place = expert_grads[:, -1].astype(jnp.int32) * ADAPTER_RANK + source_rank % ADAPTER_RANK
    placement = (source_place[:, None] == rank_range[None, :]).astype(half)
    feed = expert_down_weight.shape[1]
    bounds = [0, model_width_size, 2 * model_width_size]
    bounds += [bounds[-1] + feed, bounds[-1] + 2 * feed, bounds[-1] + 3 * feed]
    expert_pieces = [
        expert_grads[:, start:stop] for start, stop in zip(bounds, bounds[1:] + [expert_grads.shape[1] - 128])
    ]
    in_grad_a = jnp.stack([token_product(value, placement) for value in expert_pieces[:2]])
    in_grad_b = jnp.stack([token_product(placement, value) for value in expert_pieces[2:4]])
    down_grad_a = token_product(expert_pieces[4], placement)
    down_grad_b = token_product(placement, expert_pieces[5])
    return (
        layer_out,
        tokens_grad,
        attn_grad_a,
        attn_grad_b,
        jnp.transpose(summed[7]),
        summed[8][:, :experts],
        jnp.stack([jnp.transpose(summed[4]), jnp.transpose(summed[5])]),
        jnp.stack(owned[4:6]),
        jnp.transpose(owned[6]),
        summed[6],
        in_grad_a[None],
        in_grad_b[None],
        down_grad_a[None],
        down_grad_b[None],
    )


def solution(mesh):
    return jax.shard_map(
        on_device,
        mesh=mesh,
        in_specs=(
            P(("dp", "expert"), None),
            P(("dp", "expert"), None),
            P(),
            P(),
            P(None, "expert"),
            P("expert", None),
            P(),
            P(None, None, "expert"),
            P("expert", None),
            P(),
            P("expert", None, None, None),
            P("expert", None, None),
            P(("dp", "expert"), None),
            P("dp"),
            P("dp"),
            P(),
            P(),
            P(),
            P(),
            P(),
            P(),
            P(),
            P(),
            P("expert", None, None, None),
            P("expert", None, None, None),
            P("expert", None, None),
            P("expert", None, None),
        ),
        out_specs=(
            P(("dp", "expert"), None),
            P(("dp", "expert"), None),
            P(None, None, ("dp", "expert")),
            P(None, ("dp", "expert"), None),
            P(None, ("dp", "expert")),
            P(("dp", "expert"), None),
            P(None, None, ("dp", "expert")),
            P(None, ("dp", "expert"), None),
            P(None, ("dp", "expert")),
            P(("dp", "expert"), None),
            P("expert", None, None, None),
            P("expert", None, None, None),
            P("expert", None, None),
            P("expert", None, None),
        ),
        check_vma=False,
    )
```

```python
import math

import jax
import jax.numpy as jnp
from jax import lax
from jax.sharding import PartitionSpec as P

HEADS = 16
HEAD_DIM = 128
ADAPTER_RANK = 16
ADAPTER_COUNT = 8
BLOCK = 256
SEQ_MAX = 2048


NORM_EPS = 1e-06
ROPE_BASE = 1000000.0
MASKED = -1e30


def narrow_product(left_side, right_side):
    return jnp.dot(left_side, right_side, preferred_element_type=jnp.float32)


def rms_forward(values, gain_vector):
    factor = lax.rsqrt(jnp.mean(values * values, axis=-1, keepdims=True) + NORM_EPS)
    return (values * factor * gain_vector, factor)


def rms_backward(values, factor, gain_vector, upstream):
    weighted = upstream * gain_vector
    return factor * weighted - values * (factor * factor * factor) * jnp.mean(
        values * weighted, axis=-1, keepdims=True
    )


def rope_tables(positions, head_width):
    half_width = head_width // 2
    inverse = ROPE_BASE ** (-(jnp.arange(half_width).astype(jnp.float32) * 2.0 / head_width))
    angles = positions.astype(jnp.float32)[:, None] * inverse[None, :]
    return (jnp.cos(angles), jnp.sin(angles))


def rotate(values, cosine_table, sine_table, direction):
    half_width = values.shape[-1] // 2
    first_half = values[..., :half_width]
    second_half = values[..., half_width:]
    cosine_part = cosine_table[:, None, :]
    sine_part = sine_table[:, None, :] * direction
    return jnp.concatenate(
        [
            first_half * cosine_part - second_half * sine_part,
            second_half * cosine_part + first_half * sine_part,
        ],
        axis=-1,
    )


def rows_product(left_side, right_side):
    return lax.dot_general(
        left_side, right_side, (((1,), (1,)), ((), ())), preferred_element_type=jnp.float32
    )


def token_product(left_side, right_side):
    return lax.dot_general(
        left_side, right_side, (((0,), (0,)), ((), ())), preferred_element_type=jnp.float32
    )


def joint_products(left_side, right_sides):
    product = narrow_product(left_side, jnp.concatenate(right_sides, axis=1))
    pieces, at = [], 0
    for value in right_sides:
        pieces.append(product[:, at : at + value.shape[1]])
        at += value.shape[1]
    return pieces


def block_diagonal(blocks):
    rows = []
    for place, value in enumerate(blocks):
        row = [
            value if other == place else jnp.zeros((value.shape[0], side.shape[1]), value.dtype)
            for other, side in enumerate(blocks)
        ]
        rows.append(jnp.concatenate(row, axis=1))
    return jnp.concatenate(rows, axis=0)


def diagonal_blocks(product, count):
    rows, columns = product.shape[0] // count, product.shape[1] // count
    return [
        product[place * rows : (place + 1) * rows, place * columns : (place + 1) * columns]
        for place in range(count)
    ]


def row_blocks(product, count):
    rows = product.shape[0] // count
    return [product[place * rows : (place + 1) * rows] for place in range(count)]


def gated_back(gate_value, up_value, grad_hidden):
    sigmoid_gate = jax.nn.sigmoid(gate_value)
    grad_gate = grad_hidden * up_value * sigmoid_gate * (1.0 + gate_value * (1.0 - sigmoid_gate))
    grad_up = grad_hidden * gate_value * sigmoid_gate
    return jnp.concatenate([grad_gate, grad_up], axis=1).astype(jnp.bfloat16)


def head_weights(columns, owner_index, owners, slot_count, head_start, width):
    model_width_size, held = columns.shape
    groups = lax.axis_size("dp")
    group_index = lax.axis_index("dp")
    if slot_count == 1 and held == 3 * width and owners % 3 and groups & (groups - 1) == 0:
        share = model_width_size // groups
        mine = lax.dynamic_slice_in_dim(columns, group_index * share, share, 0)
        moved = jnp.stack(
            [
                lax.ppermute(
                    mine[:, step * width : (step + 1) * width],
                    "expert",
                    [(source, (3 * source + step) % owners) for source in range(owners)],
                )
                for step in range(3)
            ]
        )
        kinds = jnp.stack(
            [
                lax.dynamic_index_in_dim(moved, (owner_index + owners * kind) % 3, 0, False)
                for kind in range(3)
            ]
        )
        shares = jnp.stack(
            [kinds]
            + [
                lax.ppermute(kinds, "dp", [(source, source ^ step) for source in range(groups)])
                for step in range(1, groups)
            ]
        )
        ordered = jnp.concatenate(
            [
                lax.dynamic_index_in_dim(shares, group_index ^ place, 0, False)
                for place in range(groups)
            ],
            axis=1,
        )
        return [ordered[kind] for kind in range(3)]
    full = lax.all_gather(columns, "expert", axis=1, tiled=True)
    return [
        lax.dynamic_slice_in_dim(full, kind * model_width_size + head_start * HEAD_DIM, width, 1)
        for kind in range(3)
    ]


def spread_adapters(compact, adapter_index):
    ranks = ADAPTER_COUNT * ADAPTER_RANK
    total = jnp.zeros((ranks, compact.shape[1]), compact.dtype)
    for slot in range(adapter_index.shape[0]):
        piece = compact[slot * ADAPTER_RANK : (slot + 1) * ADAPTER_RANK]
        total = total + lax.dynamic_update_slice_in_dim(
            jnp.zeros_like(total), piece, adapter_index[slot] * ADAPTER_RANK, 0
        )
    return total


def reduce_adapters(
    partial, owned, owned_starts, owned_totals, adapter_index, owner_index, owners
):
    groups = lax.axis_size("dp")
    group_index = lax.axis_index("dp")
    slot_count = adapter_index.shape[0]
    partial_sizes = [value.shape[1] for value in partial]
    owned_sizes = [value.shape[1] for value in owned]
    partial_all = jnp.concatenate(partial, axis=1)
    owned_all = jnp.concatenate(owned, axis=1)

    def cut(values, sizes):
        pieces, at = [], 0
        for size in sizes:
            pieces.append(values[..., at : at + size])
            at += size
        return pieces

    if slot_count > 1 or ADAPTER_RANK % owners or ADAPTER_COUNT % groups or owners % (
        ADAPTER_COUNT // groups
    ):
        wide = [
            lax.dynamic_update_slice_in_dim(
                jnp.zeros((value.shape[0], total), value.dtype), value, start, 1
            )
            for value, start, total in zip(owned, owned_starts, owned_totals)
        ]
        dense = spread_adapters(jnp.concatenate([partial_all] + wide, axis=1), adapter_index)
        summed = lax.psum_scatter(dense, ("dp", "expert"), scatter_dimension=0, tiled=True)
        pieces = cut(summed, partial_sizes + owned_totals)
        return pieces[: len(partial)], pieces[len(partial) :]

    local = ADAPTER_COUNT // groups
    own_rows = ADAPTER_RANK // owners
    held = sum(partial_sizes)
    joined = jnp.concatenate([partial_all, owned_all], axis=1).astype(jnp.bfloat16)
    moved = lax.all_to_all(
        joined.reshape(owners, own_rows, joined.shape[1]),
        "expert",
        split_axis=0,
        concat_axis=0,
        tiled=True,
    )
    scattered = jnp.sum(moved[:, :, :held].astype(jnp.float32), axis=0).astype(jnp.bfloat16)
    placed = [
        jnp.transpose(value, (1, 0, 2)).reshape(own_rows, owners * size)
        for value, size in zip(cut(moved[:, :, held:], owned_sizes), owned_sizes)
    ]
    label = jnp.broadcast_to(adapter_index[:, None], (own_rows, 128)).astype(jnp.bfloat16)
    gathered = lax.all_gather(
        jnp.concatenate([scattered] + placed + [label], axis=1), "dp", axis=0
    ).astype(jnp.float32)
    labels = gathered[:, :, -1:]
    gathered = gathered[:, :, :-128]
    sums = []
    for which in range(local):
        wanted = labels == (group_index * local + which).astype(jnp.float32)
        sums.append(jnp.sum(jnp.where(wanted, gathered, 0.0), axis=0))
    sums = jnp.stack(sums).astype(jnp.bfloat16)
    arrived = []
    for step in range(local):
        piece = lax.dynamic_index_in_dim(sums, (step + owner_index) % local, 0, False)
        arrived.append(
            lax.ppermute(
                piece,
                "expert",
                [
                    (source, (step + source) % local * (owners // local) + source // local)
                    for source in range(owners)
                ],
            )
        )
    arrived = jnp.stack(arrived)
    place = owner_index // (owners // local)
    rows = jnp.concatenate(
        [
            lax.dynamic_index_in_dim(arrived, (place - which) % local, 0, False)
            for which in range(local)
        ],
        axis=0,
    )
    pieces = cut(rows.astype(jnp.float32), partial_sizes + [owners * size for size in owned_sizes])
    return pieces[: len(partial)], pieces[len(partial) :]


def on_device(
    tokens,
    cotangent,
    attention_norm_gain,
    experts_norm_gain,
    attention_query_key_value,
    attention_output_weight,
    router_projection,
    shared_gate_up_weight,
    shared_down_weight,
    shared_gate_vector,
    expert_gate_up_weight,
    expert_down_weight,
    routes,
    lengths,
    adapter_slot_index,
    attention_adapter_first,
    attention_adapter_second,
    router_adapter_first,
    router_adapter_second,
    shared_adapter_first,
    shared_adapter_second,
    shared_down_adapter_first,
    shared_down_adapter_second,
    expert_adapter_first,
    expert_adapter_second,
    expert_down_adapter_first,
    expert_down_adapter_second,
):
    count_rows, model_width_size = tokens.shape
    owners = lax.axis_size("expert")
    owner_index = lax.axis_index("expert")
    experts = router_projection.shape[1]
    top_count = routes.shape[1]
    capacity = (count_rows * top_count * 9 + 8 * experts - 1) // (8 * experts)
    group_rows = count_rows * owners
    seq_length = min(SEQ_MAX, group_rows)
    slot_count = lengths.shape[0]
    group_devices = owners // slot_count
    head_count = HEADS // group_devices
    width = head_count * HEAD_DIM
    own_slot = owner_index // group_devices
    head_start = owner_index % group_devices * head_count
    head_column = head_start * HEAD_DIM
    score_scale = 1.0 / math.sqrt(HEAD_DIM)
    half = jnp.bfloat16

    def own_rows(values):
        return lax.dynamic_slice_in_dim(values, owner_index * count_rows, count_rows, 0)

    def slot_rows(values):
        if slot_count == 1:
            return values
        return lax.dynamic_slice_in_dim(values, own_slot * seq_length, seq_length, 0)

    def group_wide(values):
        if slot_count == 1:
            return values
        return lax.dynamic_update_slice_in_dim(
            jnp.zeros((group_rows, values.shape[1]), values.dtype), values, own_slot * seq_length, 0
        )

    def slot_wide(values):
        if slot_count == 1:
            return values
        return lax.dynamic_update_slice_in_dim(
            jnp.zeros((slot_count * ADAPTER_RANK, values.shape[1]), values.dtype),
            values,
            own_slot * ADAPTER_RANK,
            0,
        )

    def slot_value(values):
        return values[0] if slot_count == 1 else lax.dynamic_index_in_dim(values, own_slot, 0, False)

    def picked_maps(maps, axis):
        return jnp.concatenate(
            [
                lax.dynamic_slice_in_dim(
                    maps, adapter_slot_index[slot] * ADAPTER_RANK, ADAPTER_RANK, axis
                )
                for slot in range(slot_count)
            ],
            axis=axis,
        )

    def scatter_rows(values):
        return lax.psum_scatter(values.astype(half), "expert", scatter_dimension=0, tiled=True)

    tokens_all = lax.all_gather(tokens, "expert", axis=0, tiled=True)
    qkv_weights = head_weights(
        attention_query_key_value, owner_index, owners, slot_count, head_start, width
    )
    routes_all = lax.all_gather(routes, "expert", axis=0, tiled=True)
    tokens_all, routes_all = lax.optimization_barrier((tokens_all, routes_all))
    upstream_all = lax.all_gather(cotangent, "expert", axis=0, tiled=True)
    if attention_output_weight.shape[0] == width:
        output_weight = attention_output_weight
    else:
        output_weight = lax.dynamic_slice_in_dim(
            lax.all_gather(attention_output_weight, "expert", axis=0, tiled=True),
            head_column,
            width,
            0,
        )

    if slot_count == 1:
        selector = None
    else:
        row_slot = jnp.arange(group_rows, dtype=jnp.int32) // seq_length
        rank_slot = jnp.arange(slot_count * ADAPTER_RANK, dtype=jnp.int32) // ADAPTER_RANK
        selector = (row_slot[:, None] == rank_slot[None, :]).astype(half)

    def chosen(values, picker):
        narrow = values.astype(half)
        return narrow if picker is None else narrow * picker

    def twice(picker):
        return None if picker is None else jnp.concatenate([picker, picker], axis=1)

    attention_adapter = slot_value(adapter_slot_index) * ADAPTER_RANK
    attention_first = lax.dynamic_slice_in_dim(
        attention_adapter_first, attention_adapter, ADAPTER_RANK, 2
    )
    attention_second = lax.dynamic_slice_in_dim(
        attention_adapter_second, attention_adapter, ADAPTER_RANK, 1
    )
    qkv_second = lax.dynamic_slice_in_dim(attention_second[:3], head_column, width, 2)
    output_first = lax.dynamic_slice_in_dim(attention_first[3], head_column, width, 0)
    output_second = attention_second[3]
    router_first = picked_maps(router_adapter_first, 1)
    router_second = picked_maps(router_adapter_second, 0)
    shared_wide = shared_down_weight.shape[0]
    shared_first = picked_maps(shared_adapter_first, 2)
    shared_second = lax.dynamic_slice_in_dim(
        picked_maps(shared_adapter_second, 1), owner_index * shared_wide, shared_wide, 2
    )
    down_first = lax.dynamic_slice_in_dim(
        picked_maps(shared_down_adapter_first, 1), owner_index * shared_wide, shared_wide, 0
    )
    down_second = picked_maps(shared_down_adapter_second, 0)
    expert_first = picked_maps(expert_adapter_first[0], 2)
    expert_second = picked_maps(expert_adapter_second[0], 1)
    expert_down_first = picked_maps(expert_down_adapter_first[0], 1)
    expert_down_second = picked_maps(expert_down_adapter_second[0], 0)

    expert_range = jnp.arange(experts, dtype=jnp.int32)
    route_hits = jnp.any(routes_all[:, :, None] == expert_range[None, None, :], axis=1)
    own_hits = jnp.any(routes_all == owner_index, axis=1)
    ranks = jnp.cumsum(own_hits.astype(jnp.int32)) - 1
    row_range = jnp.arange(experts * capacity, dtype=jnp.int32)
    placed = (ranks[None, :] == row_range[:, None]) & own_hits[None, :]
    spread = placed.astype(half)
    row_selector = None if selector is None else narrow_product(spread, selector).astype(half)

    slot_tokens = slot_rows(tokens_all).astype(jnp.float32)
    normed_first, unused = rms_forward(slot_tokens, attention_norm_gain)
    first_narrow = normed_first.astype(half)
    positions = jnp.arange(seq_length, dtype=jnp.int32)
    cosine_table, sine_table = rope_tables(positions, HEAD_DIM)
    shaped = (seq_length, head_count, HEAD_DIM)
    qkv_joined = jnp.concatenate(qkv_weights + [attention_first[kind] for kind in range(3)], axis=1)
    qkv_up = block_diagonal([qkv_second[kind] for kind in range(3)])
    projected = narrow_product(first_narrow, qkv_joined)
    attention_middle = projected[:, 3 * width :].astype(half)
    projected = projected[:, : 3 * width] + narrow_product(attention_middle, qkv_up)
    projected = [projected[:, kind * width : (kind + 1) * width] for kind in range(3)]
    query_low = rotate(projected[0].reshape(shaped), cosine_table, sine_table, 1.0).astype(half)
    key_low = rotate(projected[1].reshape(shaped), cosine_table, sine_table, 1.0).astype(half)
    value_low = projected[2].reshape(shaped).astype(half)
    allowed = ((positions // BLOCK)[None, :] <= (positions // BLOCK)[:, None]) & (
        positions < slot_value(lengths)
    )[None, :]
    scores = (
        jnp.einsum("qhd,khd->hqk", query_low, key_low, preferred_element_type=jnp.float32)
        * score_scale
    )
    scores = jnp.where(allowed[None], scores, MASKED)
    exponents = jnp.exp(scores - jnp.max(scores, axis=2, keepdims=True)) * allowed[None]
    probabilities = exponents / jnp.sum(exponents, axis=2, keepdims=True)
    probabilities_low = probabilities.astype(half)
    attended = jnp.einsum(
        "hqk,khd->qhd", probabilities_low, value_low, preferred_element_type=jnp.float32
    )
    attended_low = attended.reshape(seq_length, width).astype(half)
    attended_low, upstream_all = lax.optimization_barrier((attended_low, upstream_all))
    output_middle = narrow_product(attended_low, output_first).astype(half)
    attention_part = narrow_product(attended_low, output_weight) + narrow_product(
        output_middle, output_second
    )
    input_rows = tokens.astype(jnp.float32)
    residual_stream = input_rows + scatter_rows(group_wide(attention_part)).astype(jnp.float32)
    normed_second, factor_second = rms_forward(residual_stream, experts_norm_gain)
    second_own = normed_second.astype(half)
    second_all = lax.all_gather(second_own, "expert", axis=0, tiled=True)

    router_raw, router_plain, gate_raw = joint_products(
        second_all, [router_first, router_projection, shared_gate_vector[:, None]]
    )
    router_middle = chosen(router_raw, selector)
    router_scores = router_plain + narrow_product(router_middle, router_second)
    reach = jnp.max(jnp.where(route_hits, router_scores, MASKED), axis=1, keepdims=True)
    gate_exponents = jnp.where(route_hits, jnp.exp(jnp.minimum(router_scores - reach, 0.0)), 0.0)
    gate_weights = gate_exponents / jnp.sum(gate_exponents, axis=1, keepdims=True)
    own_gate = jnp.sum(jnp.where(expert_range[None, :] == owner_index, gate_weights, 0.0), axis=1)
    row_gate = jnp.sum(jnp.where(placed, own_gate[None, :], 0.0), axis=1, keepdims=True)
    shared_weight = jax.nn.sigmoid(gate_raw)

    expert_rows = narrow_product(spread, second_all).astype(half)
    feed = expert_down_weight.shape[1]
    expert_joined = jnp.concatenate(
        [expert_gate_up_weight[0, 0], expert_gate_up_weight[0, 1], expert_first[0], expert_first[1]],
        axis=1,
    )
    expert_up = block_diagonal([expert_second[0], expert_second[1]])
    expert_pre = narrow_product(expert_rows, expert_joined)
    expert_middle = chosen(expert_pre[:, 2 * feed :], twice(row_selector))
    expert_pre = expert_pre[:, : 2 * feed] + narrow_product(expert_middle, expert_up)
    expert_pre = (expert_pre[:, :feed], expert_pre[:, feed:])
    expert_hidden = (jax.nn.silu(expert_pre[0]) * expert_pre[1]).astype(half)
    expert_down_middle = chosen(narrow_product(expert_hidden, expert_down_first), row_selector)
    expert_result = (
        narrow_product(expert_hidden, expert_down_weight[0])
        + narrow_product(expert_down_middle, expert_down_second)
    ).astype(half)

    shared_joined = jnp.concatenate(
        [shared_gate_up_weight[0], shared_gate_up_weight[1], shared_first[0], shared_first[1]], axis=1
    )
    shared_up = block_diagonal([shared_second[0], shared_second[1]])
    shared_pre = narrow_product(second_all, shared_joined)
    shared_middle = chosen(shared_pre[:, 2 * shared_wide :], twice(selector))
    shared_pre = shared_pre[:, : 2 * shared_wide] + narrow_product(shared_middle, shared_up)
    shared_pre = (shared_pre[:, :shared_wide], shared_pre[:, shared_wide:])
    shared_hidden = (jax.nn.silu(shared_pre[0]) * shared_pre[1]).astype(half)
    down_middle = chosen(narrow_product(shared_hidden, down_first), selector)
    shared_part = narrow_product(shared_hidden, shared_down_weight) + narrow_product(
        down_middle, down_second
    )
    layer_part = (
        token_product(spread, (row_gate * expert_result.astype(jnp.float32)).astype(half))
        + shared_weight * shared_part
    )
    layer_sum = scatter_rows(layer_part)
    upstream_wide = upstream_all.astype(jnp.float32)
    shared_dot = jnp.sum(upstream_wide * shared_part, axis=1)

    upstream_rows = narrow_product(spread, upstream_all)
    row_dot = jnp.sum(upstream_rows * expert_result.astype(jnp.float32), axis=1, keepdims=True)
    gate_dot = jnp.sum(jnp.where(placed, row_dot, 0.0), axis=0)
    expert_upstream = (row_gate * upstream_rows).astype(half)
    expert_down_joined = jnp.concatenate([expert_down_weight[0], expert_down_second], axis=0)
    expert_grad_hidden = rows_product(expert_upstream, expert_down_joined)
    expert_down_inner = chosen(expert_grad_hidden[:, feed:], row_selector)
    expert_grad_hidden = expert_grad_hidden[:, :feed] + rows_product(
        expert_down_inner, expert_down_first
    )
    expert_grad_pre = gated_back(expert_pre[0], expert_pre[1], expert_grad_hidden)
    expert_inner = chosen(rows_product(expert_grad_pre, expert_up), twice(row_selector))
    copy_grad = rows_product(
        jnp.concatenate([expert_grad_pre, expert_inner], axis=1), expert_joined
    ).astype(half)

    value_grads = (shared_weight * upstream_wide).astype(half)
    down_joined = jnp.concatenate([shared_down_weight, down_second], axis=0)
    shared_grad_hidden = rows_product(value_grads, down_joined)
    down_inner = chosen(shared_grad_hidden[:, shared_wide:], selector)
    shared_grad_hidden = shared_grad_hidden[:, :shared_wide] + rows_product(down_inner, down_first)
    shared_grad_pre = gated_back(shared_pre[0], shared_pre[1], shared_grad_hidden)
    shared_inner = chosen(rows_product(shared_grad_pre, shared_up), twice(selector))
    copy_grad, layer_sum = lax.optimization_barrier((copy_grad, layer_sum))
    second_part = token_product(spread, copy_grad) + rows_product(
        jnp.concatenate([shared_grad_pre, shared_inner], axis=1), shared_joined
    )
    dots = jnp.concatenate(
        [
            jnp.where(expert_range[:, None] == owner_index, gate_dot[None, :], 0.0),
            shared_dot[None, :],
            jnp.zeros((7, group_rows), jnp.float32),
        ],
        axis=0,
    )
    own_dots = jnp.transpose(lax.psum_scatter(dots, "expert", scatter_dimension=1, tiled=True))
    second_sum = scatter_rows(second_part).astype(jnp.float32)
    own_weights = own_rows(gate_weights)
    gate_grads = own_dots[:, :experts]
    centered = own_weights * (
        gate_grads - jnp.sum(own_weights * gate_grads, axis=1, keepdims=True)
    )
    logit_grads = centered.astype(half)
    own_selector = None if selector is None else own_rows(selector)
    router_inner = chosen(rows_product(logit_grads, router_second), own_selector)
    own_shared_weight = own_rows(shared_weight)
    weight_grads = own_dots[:, experts : experts + 1] * own_shared_weight * (1.0 - own_shared_weight)
    second_grad = (
        second_sum
        + rows_product(logit_grads, router_projection)
        + rows_product(router_inner, router_first)
        + weight_grads * shared_gate_vector.astype(jnp.float32)[None, :]
    )
    residual_grad = cotangent.astype(jnp.float32) + rms_backward(
        residual_stream, factor_second, experts_norm_gain, second_grad
    )
    output_upstream = slot_rows(
        lax.all_gather(residual_grad.astype(half), "expert", axis=0, tiled=True)
    )

    wide_grads = jnp.concatenate(
        [
            *row_blocks(token_product(expert_inner, expert_rows), 2),
            *diagonal_blocks(token_product(expert_middle, expert_grad_pre), 2),
            token_product(expert_down_inner, expert_hidden),
            token_product(expert_down_middle, expert_upstream),
            jnp.broadcast_to(
                jnp.repeat(adapter_slot_index, ADAPTER_RANK).astype(jnp.float32)[:, None],
                (slot_count * ADAPTER_RANK, 128),
            ),
        ],
        axis=1,
    ).astype(half)
    wide_grads, output_upstream = lax.optimization_barrier((wide_grads, output_upstream))

    output_inner = rows_product(output_upstream, output_second).astype(half)
    attended_grad = (
        (rows_product(output_upstream, output_weight) + rows_product(output_inner, output_first))
        .astype(half)
        .reshape(shaped)
    )
    row_delta = jnp.transpose(jnp.sum(attended_grad.astype(jnp.float32) * attended, axis=2))
    prob_grads = jnp.einsum(
        "qhd,khd->hqk", attended_grad, value_low, preferred_element_type=jnp.float32
    )
    score_grad = (probabilities * (prob_grads - row_delta[:, :, None])).astype(half)
    query_grad = (
        jnp.einsum("hqk,khd->qhd", score_grad, key_low, preferred_element_type=jnp.float32)
        * score_scale
    )
    key_grad = (
        jnp.einsum("hqk,qhd->khd", score_grad, query_low, preferred_element_type=jnp.float32)
        * score_scale
    )
    value_grad = jnp.einsum(
        "hqk,qhd->khd", probabilities_low, attended_grad, preferred_element_type=jnp.float32
    )
    pre_grads = jnp.concatenate(
        [
            rotate(query_grad, cosine_table, sine_table, -1.0).reshape(seq_length, width),
            rotate(key_grad, cosine_table, sine_table, -1.0).reshape(seq_length, width),
            value_grad.reshape(seq_length, width),
        ],
        axis=1,
    ).astype(half)
    qkv_inner = rows_product(pre_grads, qkv_up).astype(half)
    first_part = rows_product(jnp.concatenate([pre_grads, qkv_inner], axis=1), qkv_joined)
    first_grad = scatter_rows(group_wide(first_part)).astype(jnp.float32)
    unused, factor_first = rms_forward(input_rows, attention_norm_gain)
    tokens_grad = residual_grad + rms_backward(
        input_rows, factor_first, attention_norm_gain, first_grad
    )
    layer_out = (residual_stream + layer_sum.astype(jnp.float32)).astype(half)

    own_router_middle = own_rows(router_middle)
    router_grad_b = token_product(own_router_middle, logit_grads)
    spare = -experts % 128
    summed, owned = reduce_adapters(
        [slot_wide(value) for value in row_blocks(token_product(qkv_inner, first_narrow), 3)]
        + [slot_wide(token_product(output_middle, output_upstream))]
        + row_blocks(token_product(shared_inner, second_all), 2)
        + [
            token_product(down_middle, value_grads),
            token_product(router_inner, second_own),
            jnp.pad(router_grad_b, ((0, 0), (0, spare))),
        ],
        [
            slot_wide(value)
            for value in diagonal_blocks(token_product(attention_middle, pre_grads), 3)
        ]
        + [slot_wide(token_product(output_inner, attended_low))]
        + diagonal_blocks(token_product(shared_middle, shared_grad_pre), 2)
        + [token_product(down_inner, shared_hidden)],
        [head_column] * 4 + [owner_index * shared_wide] * 3,
        [model_width_size] * 4 + [owners * shared_wide] * 3,
        adapter_slot_index,
        owner_index,
        owners,
    )
    attn_grad_a = jnp.stack([jnp.transpose(value) for value in summed[:3] + owned[3:4]])
    attn_grad_b = jnp.stack(owned[:3] + summed[3:4])

    expert_grads = lax.all_gather(wide_grads, "dp", axis=0, tiled=True)
    rank_range = jnp.arange(ADAPTER_COUNT * ADAPTER_RANK, dtype=jnp.int32)
    source_rank = jnp.arange(expert_grads.shape[0], dtype=jnp.int32)
    source_place = expert_grads[:, -1].astype(jnp.int32) * ADAPTER_RANK + source_rank % ADAPTER_RANK
    placement = (source_place[:, None] == rank_range[None, :]).astype(half)
    bounds = [0, model_width_size, 2 * model_width_size]
    bounds += [bounds[-1] + feed, bounds[-1] + 2 * feed, bounds[-1] + 3 * feed]
    expert_pieces = [
        expert_grads[:, start:stop] for start, stop in zip(bounds, bounds[1:] + [expert_grads.shape[1] - 128])
    ]
    in_grad_a = jnp.stack([token_product(value, placement) for value in expert_pieces[:2]])
    in_grad_b = jnp.stack([token_product(placement, value) for value in expert_pieces[2:4]])
    down_grad_a = token_product(expert_pieces[4], placement)
    down_grad_b = token_product(placement, expert_pieces[5])
    return (
        layer_out,
        tokens_grad,
        attn_grad_a,
        attn_grad_b,
        jnp.transpose(summed[7]),
        summed[8][:, :experts],
        jnp.stack([jnp.transpose(summed[4]), jnp.transpose(summed[5])]),
        jnp.stack(owned[4:6]),
        jnp.transpose(owned[6]),
        summed[6],
        in_grad_a[None],
        in_grad_b[None],
        down_grad_a[None],
        down_grad_b[None],
    )


def solution(mesh):
    return jax.shard_map(
        on_device,
        mesh=mesh,
        in_specs=(
            P(("dp", "expert"), None),
            P(("dp", "expert"), None),
            P(),
            P(),
            P(None, "expert"),
            P("expert", None),
            P(),
            P(None, None, "expert"),
            P("expert", None),
            P(),
            P("expert", None, None, None),
            P("expert", None, None),
            P(("dp", "expert"), None),
            P("dp"),
            P("dp"),
            P(),
            P(),
            P(),
            P(),
            P(),
            P(),
            P(),
            P(),
            P("expert", None, None, None),
            P("expert", None, None, None),
            P("expert", None, None),
            P("expert", None, None),
        ),
        out_specs=(
            P(("dp", "expert"), None),
            P(("dp", "expert"), None),
            P(None, None, ("dp", "expert")),
            P(None, ("dp", "expert"), None),
            P(None, ("dp", "expert")),
            P(("dp", "expert"), None),
            P(None, None, ("dp", "expert")),
            P(None, ("dp", "expert"), None),
            P(None, ("dp", "expert")),
            P(("dp", "expert"), None),
            P("expert", None, None, None),
            P("expert", None, None, None),
            P("expert", None, None),
            P("expert", None, None),
        ),
        check_vma=False,
    )
```

```python
import functools
import math

import jax
import jax.numpy as jnp
from jax import lax
from jax.experimental import pallas as pl
from jax.experimental.pallas import tpu as pltpu
from jax.sharding import PartitionSpec as P

HEADS = 16
HEAD_DIM = 128
ADAPTER_RANK = 16
ADAPTER_COUNT = 8
BLOCK = 256
SEQ_MAX = 2048


NORM_EPS = 1e-06
ROPE_BASE = 1000000.0
MASKED = -1e30


def narrow_product(left_side, right_side):
    return jnp.dot(left_side, right_side, preferred_element_type=jnp.float32)


def rms_forward(values, gain_vector):
    factor = lax.rsqrt(jnp.mean(values * values, axis=-1, keepdims=True) + NORM_EPS)
    return (values * factor * gain_vector, factor)


def rms_backward(values, factor, gain_vector, upstream):
    weighted = upstream * gain_vector
    return factor * weighted - values * (factor * factor * factor) * jnp.mean(
        values * weighted, axis=-1, keepdims=True
    )


def rope_tables(positions, head_width):
    half_width = head_width // 2
    inverse = ROPE_BASE ** (-(jnp.arange(half_width).astype(jnp.float32) * 2.0 / head_width))
    angles = positions.astype(jnp.float32)[:, None] * inverse[None, :]
    return (jnp.cos(angles), jnp.sin(angles))


def turn(values, cosine_table, sine_table):
    return values * cosine_table + pltpu.roll(values, HEAD_DIM // 2, 1) * sine_table


def head_product(left_side, right_side, left_dim, right_dim):
    return lax.dot_general(
        left_side,
        right_side,
        (((left_dim,), (right_dim,)), ((), ())),
        preferred_element_type=jnp.float32,
    )


def block_probabilities(query_rows, key_rows, live, score_scale):
    scores = head_product(query_rows, key_rows, 1, 1) * score_scale
    scores = jnp.where(live, scores, MASKED)
    exponents = jnp.exp(scores - jnp.max(scores, axis=1, keepdims=True))
    return exponents / jnp.sum(exponents, axis=1, keepdims=True)


def attention_forward(
    score_scale, length_ref, q_ref, k_ref, v_ref, cos_ref, sin_ref, out_ref, ql_ref, kl_ref, vl_ref
):
    rows = q_ref.shape[0]
    cosine_table, sine_table = cos_ref[...], sin_ref[...]
    ql_ref[...] = turn(q_ref[...], cosine_table, sine_table).astype(jnp.bfloat16)
    kl_ref[...] = turn(k_ref[...], cosine_table, sine_table).astype(jnp.bfloat16)
    vl_ref[...] = v_ref[...].astype(jnp.bfloat16)
    for start in range(0, rows, BLOCK):
        stop = start + BLOCK
        live = lax.broadcasted_iota(jnp.int32, (BLOCK, stop), 1) < length_ref[0]
        probabilities = block_probabilities(
            ql_ref[start:stop, :], kl_ref[:stop, :], live, score_scale
        )
        out_ref[start:stop, :] = head_product(
            probabilities.astype(jnp.bfloat16), vl_ref[:stop, :], 1, 0
        ).astype(jnp.bfloat16)


def attention_backward(
    score_scale,
    length_ref,
    q_ref,
    k_ref,
    v_ref,
    grad_ref,
    cos_ref,
    sin_ref,
    dq_ref,
    dk_ref,
    dv_ref,
    key_sum,
    value_sum,
):
    rows = q_ref.shape[0]
    cosine_table, sine_table = cos_ref[...], sin_ref[...]
    key_sum[...] = jnp.zeros_like(key_sum)
    value_sum[...] = jnp.zeros_like(value_sum)
    for start in range(0, rows, BLOCK):
        stop = start + BLOCK
        live = lax.broadcasted_iota(jnp.int32, (BLOCK, stop), 1) < length_ref[0]
        query_rows, grad_rows = q_ref[start:stop, :], grad_ref[start:stop, :]
        probabilities = block_probabilities(query_rows, k_ref[:stop, :], live, score_scale)
        narrow = probabilities.astype(jnp.bfloat16)
        prob_grads = head_product(grad_rows, v_ref[:stop, :], 1, 1)
        delta = jnp.sum(narrow.astype(jnp.float32) * prob_grads, axis=1, keepdims=True)
        score_grads = (probabilities * (prob_grads - delta)).astype(jnp.bfloat16)
        query_grads = head_product(score_grads, k_ref[:stop, :], 1, 0) * score_scale
        dq_ref[start:stop, :] = turn(
            query_grads, cosine_table[start:stop, :], -sine_table[start:stop, :]
        ).astype(jnp.bfloat16)
        key_sum[:stop, :] += head_product(score_grads, query_rows, 0, 0)
        value_sum[:stop, :] += head_product(narrow, grad_rows, 0, 0)
    dk_ref[...] = turn(key_sum[...] * score_scale, cosine_table, -sine_table).astype(jnp.bfloat16)
    dv_ref[...] = value_sum[...].astype(jnp.bfloat16)


def head_attention(query, key, value, length, cosine_table, sine_table, score_scale):
    rows, width = query.shape
    head = pl.BlockSpec((rows, HEAD_DIM), lambda place: (0, place))
    table = pl.BlockSpec((rows, HEAD_DIM), lambda place: (0, 0))
    shape = jax.ShapeDtypeStruct((rows, width), jnp.bfloat16)
    return pl.pallas_call(
        functools.partial(attention_forward, score_scale),
        grid=(width // HEAD_DIM,),
        in_specs=[pl.BlockSpec(memory_space=pltpu.SMEM), head, head, head, table, table],
        out_specs=[head] * 4,
        out_shape=[shape] * 4,
        compiler_params=pltpu.CompilerParams(vmem_limit_bytes=48 * 1024 * 1024),
        cost_estimate=pl.CostEstimate(
            flops=3 * rows * rows * width, bytes_accessed=24 * rows * width, transcendentals=rows * rows
        ),
        name="head_attention",
    )(length, query, key, value, cosine_table, sine_table)


def head_attention_back(query, key, value, grad, length, cosine_table, sine_table, score_scale):
    rows, width = query.shape
    head = pl.BlockSpec((rows, HEAD_DIM), lambda place: (0, place))
    table = pl.BlockSpec((rows, HEAD_DIM), lambda place: (0, 0))
    shape = jax.ShapeDtypeStruct((rows, width), jnp.bfloat16)
    return pl.pallas_call(
        functools.partial(attention_backward, score_scale),
        grid=(width // HEAD_DIM,),
        in_specs=[pl.BlockSpec(memory_space=pltpu.SMEM)] + [head] * 4 + [table, table],
        out_specs=[head] * 3,
        out_shape=[shape] * 3,
        scratch_shapes=[
            pltpu.VMEM((rows, HEAD_DIM), jnp.float32),
            pltpu.VMEM((rows, HEAD_DIM), jnp.float32),
        ],
        compiler_params=pltpu.CompilerParams(vmem_limit_bytes=48 * 1024 * 1024),
        cost_estimate=pl.CostEstimate(
            flops=7 * rows * rows * width, bytes_accessed=16 * rows * width, transcendentals=rows * rows
        ),
        name="head_attention_back",
    )(length, query, key, value, grad, cosine_table, sine_table)


def rows_product(left_side, right_side):
    return lax.dot_general(
        left_side, right_side, (((1,), (1,)), ((), ())), preferred_element_type=jnp.float32
    )


def token_product(left_side, right_side):
    return lax.dot_general(
        left_side, right_side, (((0,), (0,)), ((), ())), preferred_element_type=jnp.float32
    )


def joint_products(left_side, right_sides):
    product = narrow_product(left_side, jnp.concatenate(right_sides, axis=1))
    pieces, at = [], 0
    for value in right_sides:
        pieces.append(product[:, at : at + value.shape[1]])
        at += value.shape[1]
    return pieces


def block_diagonal(blocks):
    rows = []
    for place, value in enumerate(blocks):
        row = [
            value if other == place else jnp.zeros((value.shape[0], side.shape[1]), value.dtype)
            for other, side in enumerate(blocks)
        ]
        rows.append(jnp.concatenate(row, axis=1))
    return jnp.concatenate(rows, axis=0)


def diagonal_blocks(product, count):
    rows, columns = product.shape[0] // count, product.shape[1] // count
    return [
        product[place * rows : (place + 1) * rows, place * columns : (place + 1) * columns]
        for place in range(count)
    ]


def row_blocks(product, count):
    rows = product.shape[0] // count
    return [product[place * rows : (place + 1) * rows] for place in range(count)]


def gated_back(gate_value, up_value, grad_hidden):
    sigmoid_gate = jax.nn.sigmoid(gate_value)
    grad_gate = grad_hidden * up_value * sigmoid_gate * (1.0 + gate_value * (1.0 - sigmoid_gate))
    grad_up = grad_hidden * gate_value * sigmoid_gate
    return jnp.concatenate([grad_gate, grad_up], axis=1).astype(jnp.bfloat16)


def head_weights(columns, owner_index, owners, slot_count, head_start, width):
    model_width_size, held = columns.shape
    groups = lax.axis_size("dp")
    group_index = lax.axis_index("dp")
    if slot_count == 1 and held == 3 * width and owners % 3 and groups & (groups - 1) == 0:
        share = model_width_size // groups
        mine = lax.dynamic_slice_in_dim(columns, group_index * share, share, 0)
        moved = jnp.stack(
            [
                lax.ppermute(
                    mine[:, step * width : (step + 1) * width],
                    "expert",
                    [(source, (3 * source + step) % owners) for source in range(owners)],
                )
                for step in range(3)
            ]
        )
        kinds = jnp.stack(
            [
                lax.dynamic_index_in_dim(moved, (owner_index + owners * kind) % 3, 0, False)
                for kind in range(3)
            ]
        )
        shares = jnp.stack(
            [kinds]
            + [
                lax.ppermute(kinds, "dp", [(source, source ^ step) for source in range(groups)])
                for step in range(1, groups)
            ]
        )
        ordered = jnp.concatenate(
            [
                lax.dynamic_index_in_dim(shares, group_index ^ place, 0, False)
                for place in range(groups)
            ],
            axis=1,
        )
        return [ordered[kind] for kind in range(3)]
    full = lax.all_gather(columns, "expert", axis=1, tiled=True)
    return [
        lax.dynamic_slice_in_dim(full, kind * model_width_size + head_start * HEAD_DIM, width, 1)
        for kind in range(3)
    ]


def spread_adapters(compact, adapter_index):
    ranks = ADAPTER_COUNT * ADAPTER_RANK
    total = jnp.zeros((ranks, compact.shape[1]), compact.dtype)
    for slot in range(adapter_index.shape[0]):
        piece = compact[slot * ADAPTER_RANK : (slot + 1) * ADAPTER_RANK]
        total = total + lax.dynamic_update_slice_in_dim(
            jnp.zeros_like(total), piece, adapter_index[slot] * ADAPTER_RANK, 0
        )
    return total


def reduce_adapters(
    partial, owned, owned_starts, owned_totals, adapter_index, owner_index, owners, ahead
):
    groups = lax.axis_size("dp")
    group_index = lax.axis_index("dp")
    slot_count = adapter_index.shape[0]
    partial_sizes = [value.shape[1] for value in partial]
    owned_sizes = [value.shape[1] for value in owned]
    partial_all = jnp.concatenate(partial, axis=1)
    owned_all = jnp.concatenate(owned, axis=1)

    def cut(values, sizes):
        pieces, at = [], 0
        for size in sizes:
            pieces.append(values[..., at : at + size])
            at += size
        return pieces

    if slot_count > 1 or ADAPTER_RANK % owners or ADAPTER_COUNT % groups or owners % (
        ADAPTER_COUNT // groups
    ):
        wide = [
            lax.dynamic_update_slice_in_dim(
                jnp.zeros((value.shape[0], total), value.dtype), value, start, 1
            )
            for value, start, total in zip(owned, owned_starts, owned_totals)
        ]
        dense = spread_adapters(jnp.concatenate([partial_all] + wide, axis=1), adapter_index)
        summed = lax.psum_scatter(dense, ("dp", "expert"), scatter_dimension=0, tiled=True)
        pieces = cut(summed, partial_sizes + owned_totals)
        return pieces[: len(partial)], pieces[len(partial) :], ahead

    local = ADAPTER_COUNT // groups
    own_rows = ADAPTER_RANK // owners
    held = sum(partial_sizes)
    joined = jnp.concatenate([partial_all, owned_all], axis=1).astype(jnp.bfloat16)
    joined, ahead = lax.optimization_barrier((joined, ahead))
    moved = lax.all_to_all(
        joined.reshape(owners, own_rows, joined.shape[1]),
        "expert",
        split_axis=0,
        concat_axis=0,
        tiled=True,
    )
    scattered = jnp.sum(moved[:, :, :held].astype(jnp.float32), axis=0).astype(jnp.bfloat16)
    placed = [
        jnp.transpose(value, (1, 0, 2)).reshape(own_rows, owners * size)
        for value, size in zip(cut(moved[:, :, held:], owned_sizes), owned_sizes)
    ]
    label = jnp.broadcast_to(adapter_index[:, None], (own_rows, 128)).astype(jnp.bfloat16)
    gathered = lax.all_gather(
        jnp.concatenate([scattered] + placed + [label], axis=1), "dp", axis=0
    ).astype(jnp.float32)
    labels = gathered[:, :, -1:]
    gathered = gathered[:, :, :-128]
    sums = []
    for which in range(local):
        wanted = labels == (group_index * local + which).astype(jnp.float32)
        sums.append(jnp.sum(jnp.where(wanted, gathered, 0.0), axis=0))
    sums = jnp.stack(sums).astype(jnp.bfloat16)
    arrived = []
    for step in range(local):
        piece = lax.dynamic_index_in_dim(sums, (step + owner_index) % local, 0, False)
        arrived.append(
            lax.ppermute(
                piece,
                "expert",
                [
                    (source, (step + source) % local * (owners // local) + source // local)
                    for source in range(owners)
                ],
            )
        )
    arrived = jnp.stack(arrived)
    place = owner_index // (owners // local)
    rows = jnp.concatenate(
        [
            lax.dynamic_index_in_dim(arrived, (place - which) % local, 0, False)
            for which in range(local)
        ],
        axis=0,
    )
    pieces = cut(rows.astype(jnp.float32), partial_sizes + [owners * size for size in owned_sizes])
    return pieces[: len(partial)], pieces[len(partial) :], ahead


def on_device(
    tokens,
    cotangent,
    attention_norm_gain,
    experts_norm_gain,
    attention_query_key_value,
    attention_output_weight,
    router_projection,
    shared_gate_up_weight,
    shared_down_weight,
    shared_gate_vector,
    expert_gate_up_weight,
    expert_down_weight,
    routes,
    lengths,
    adapter_slot_index,
    attention_adapter_first,
    attention_adapter_second,
    router_adapter_first,
    router_adapter_second,
    shared_adapter_first,
    shared_adapter_second,
    shared_down_adapter_first,
    shared_down_adapter_second,
    expert_adapter_first,
    expert_adapter_second,
    expert_down_adapter_first,
    expert_down_adapter_second,
):
    count_rows, model_width_size = tokens.shape
    owners = lax.axis_size("expert")
    owner_index = lax.axis_index("expert")
    experts = router_projection.shape[1]
    top_count = routes.shape[1]
    capacity = (count_rows * top_count * 9 + 8 * experts - 1) // (8 * experts)
    group_rows = count_rows * owners
    seq_length = min(SEQ_MAX, group_rows)
    slot_count = lengths.shape[0]
    group_devices = owners // slot_count
    head_count = HEADS // group_devices
    width = head_count * HEAD_DIM
    own_slot = owner_index // group_devices
    head_start = owner_index % group_devices * head_count
    head_column = head_start * HEAD_DIM
    score_scale = 1.0 / math.sqrt(HEAD_DIM)
    half = jnp.bfloat16

    def own_rows(values):
        return lax.dynamic_slice_in_dim(values, owner_index * count_rows, count_rows, 0)

    def slot_rows(values):
        if slot_count == 1:
            return values
        return lax.dynamic_slice_in_dim(values, own_slot * seq_length, seq_length, 0)

    def group_wide(values):
        if slot_count == 1:
            return values
        return lax.dynamic_update_slice_in_dim(
            jnp.zeros((group_rows, values.shape[1]), values.dtype), values, own_slot * seq_length, 0
        )

    def slot_wide(values):
        if slot_count == 1:
            return values
        return lax.dynamic_update_slice_in_dim(
            jnp.zeros((slot_count * ADAPTER_RANK, values.shape[1]), values.dtype),
            values,
            own_slot * ADAPTER_RANK,
            0,
        )

    def slot_value(values):
        return values[0] if slot_count == 1 else lax.dynamic_index_in_dim(values, own_slot, 0, False)

    def picked_maps(maps, axis):
        return jnp.concatenate(
            [
                lax.dynamic_slice_in_dim(
                    maps, adapter_slot_index[slot] * ADAPTER_RANK, ADAPTER_RANK, axis
                )
                for slot in range(slot_count)
            ],
            axis=axis,
        )

    def scatter_rows(values):
        return lax.psum_scatter(values.astype(half), "expert", scatter_dimension=0, tiled=True)

    tokens_all = lax.all_gather(tokens, "expert", axis=0, tiled=True)
    qkv_weights = head_weights(
        attention_query_key_value, owner_index, owners, slot_count, head_start, width
    )
    routes_all = lax.all_gather(routes, "expert", axis=0, tiled=True)
    tokens_all, routes_all = lax.optimization_barrier((tokens_all, routes_all))
    upstream_all = lax.all_gather(cotangent, "expert", axis=0, tiled=True)
    if attention_output_weight.shape[0] == width:
        output_weight = attention_output_weight
    else:
        output_weight = lax.dynamic_slice_in_dim(
            lax.all_gather(attention_output_weight, "expert", axis=0, tiled=True),
            head_column,
            width,
            0,
        )

    if slot_count == 1:
        selector = None
    else:
        row_slot = jnp.arange(group_rows, dtype=jnp.int32) // seq_length
        rank_slot = jnp.arange(slot_count * ADAPTER_RANK, dtype=jnp.int32) // ADAPTER_RANK
        selector = (row_slot[:, None] == rank_slot[None, :]).astype(half)

    def chosen(values, picker):
        narrow = values.astype(half)
        return narrow if picker is None else narrow * picker

    def twice(picker):
        return None if picker is None else jnp.concatenate([picker, picker], axis=1)

    attention_adapter = slot_value(adapter_slot_index) * ADAPTER_RANK
    attention_first = lax.dynamic_slice_in_dim(
        attention_adapter_first, attention_adapter, ADAPTER_RANK, 2
    )
    attention_second = lax.dynamic_slice_in_dim(
        attention_adapter_second, attention_adapter, ADAPTER_RANK, 1
    )
    qkv_second = lax.dynamic_slice_in_dim(attention_second[:3], head_column, width, 2)
    output_first = lax.dynamic_slice_in_dim(attention_first[3], head_column, width, 0)
    output_second = attention_second[3]
    router_first = picked_maps(router_adapter_first, 1)
    router_second = picked_maps(router_adapter_second, 0)
    shared_wide = shared_down_weight.shape[0]
    shared_first = picked_maps(shared_adapter_first, 2)
    shared_second = lax.dynamic_slice_in_dim(
        picked_maps(shared_adapter_second, 1), owner_index * shared_wide, shared_wide, 2
    )
    down_first = lax.dynamic_slice_in_dim(
        picked_maps(shared_down_adapter_first, 1), owner_index * shared_wide, shared_wide, 0
    )
    down_second = picked_maps(shared_down_adapter_second, 0)
    expert_first = picked_maps(expert_adapter_first[0], 2)
    expert_second = picked_maps(expert_adapter_second[0], 1)
    expert_down_first = picked_maps(expert_down_adapter_first[0], 1)
    expert_down_second = picked_maps(expert_down_adapter_second[0], 0)

    expert_range = jnp.arange(experts, dtype=jnp.int32)
    route_hits = jnp.any(routes_all[:, :, None] == expert_range[None, None, :], axis=1)
    own_hits = jnp.any(routes_all == owner_index, axis=1)
    ranks = jnp.cumsum(own_hits.astype(jnp.int32)) - 1
    row_range = jnp.arange(experts * capacity, dtype=jnp.int32)
    placed = (ranks[None, :] == row_range[:, None]) & own_hits[None, :]
    spread = placed.astype(half)
    row_selector = None if selector is None else narrow_product(spread, selector).astype(half)

    slot_tokens = slot_rows(tokens_all).astype(jnp.float32)
    normed_first, unused = rms_forward(slot_tokens, attention_norm_gain)
    first_narrow = normed_first.astype(half)
    positions = jnp.arange(seq_length, dtype=jnp.int32)
    cosine_table, sine_table = rope_tables(positions, HEAD_DIM)
    cosine_table = jnp.concatenate([cosine_table, cosine_table], axis=1)
    sine_table = jnp.concatenate([-sine_table, sine_table], axis=1)
    length = slot_value(lengths).reshape(1)
    qkv_joined = jnp.concatenate(qkv_weights + [attention_first[kind] for kind in range(3)], axis=1)
    qkv_up = block_diagonal([qkv_second[kind] for kind in range(3)])
    projected = narrow_product(first_narrow, qkv_joined)
    attention_middle = projected[:, 3 * width :].astype(half)
    projected = projected[:, : 3 * width] + narrow_product(attention_middle, qkv_up)
    projected = [projected[:, kind * width : (kind + 1) * width] for kind in range(3)]
    attended_low, query_low, key_low, value_low = head_attention(
        *projected, length, cosine_table, sine_table, score_scale
    )
    attended_low, upstream_all = lax.optimization_barrier((attended_low, upstream_all))
    output_middle = narrow_product(attended_low, output_first).astype(half)
    attention_part = narrow_product(attended_low, output_weight) + narrow_product(
        output_middle, output_second
    )
    input_rows = tokens.astype(jnp.float32)
    residual_stream = input_rows + scatter_rows(group_wide(attention_part)).astype(jnp.float32)
    normed_second, factor_second = rms_forward(residual_stream, experts_norm_gain)
    second_own = normed_second.astype(half)
    second_all = lax.all_gather(second_own, "expert", axis=0, tiled=True)

    router_raw, router_plain, gate_raw = joint_products(
        second_all, [router_first, router_projection, shared_gate_vector[:, None]]
    )
    router_middle = chosen(router_raw, selector)
    router_scores = router_plain + narrow_product(router_middle, router_second)
    reach = jnp.max(jnp.where(route_hits, router_scores, MASKED), axis=1, keepdims=True)
    gate_exponents = jnp.where(route_hits, jnp.exp(jnp.minimum(router_scores - reach, 0.0)), 0.0)
    gate_weights = gate_exponents / jnp.sum(gate_exponents, axis=1, keepdims=True)
    own_gate = jnp.sum(jnp.where(expert_range[None, :] == owner_index, gate_weights, 0.0), axis=1)
    row_gate = jnp.sum(jnp.where(placed, own_gate[None, :], 0.0), axis=1, keepdims=True)
    shared_weight = jax.nn.sigmoid(gate_raw)

    expert_rows = narrow_product(spread, second_all).astype(half)
    feed = expert_down_weight.shape[1]
    expert_joined = jnp.concatenate(
        [expert_gate_up_weight[0, 0], expert_gate_up_weight[0, 1], expert_first[0], expert_first[1]],
        axis=1,
    )
    expert_up = block_diagonal([expert_second[0], expert_second[1]])
    expert_pre = narrow_product(expert_rows, expert_joined)
    expert_middle = chosen(expert_pre[:, 2 * feed :], twice(row_selector))
    expert_pre = expert_pre[:, : 2 * feed] + narrow_product(expert_middle, expert_up)
    expert_pre = (expert_pre[:, :feed], expert_pre[:, feed:])
    expert_hidden = (jax.nn.silu(expert_pre[0]) * expert_pre[1]).astype(half)
    expert_down_middle = chosen(narrow_product(expert_hidden, expert_down_first), row_selector)
    expert_result = (
        narrow_product(expert_hidden, expert_down_weight[0])
        + narrow_product(expert_down_middle, expert_down_second)
    ).astype(half)

    shared_joined = jnp.concatenate(
        [shared_gate_up_weight[0], shared_gate_up_weight[1], shared_first[0], shared_first[1]], axis=1
    )
    shared_up = block_diagonal([shared_second[0], shared_second[1]])
    shared_pre = narrow_product(second_all, shared_joined)
    shared_middle = chosen(shared_pre[:, 2 * shared_wide :], twice(selector))
    shared_pre = shared_pre[:, : 2 * shared_wide] + narrow_product(shared_middle, shared_up)
    shared_pre = (shared_pre[:, :shared_wide], shared_pre[:, shared_wide:])
    shared_hidden = (jax.nn.silu(shared_pre[0]) * shared_pre[1]).astype(half)
    down_middle = chosen(narrow_product(shared_hidden, down_first), selector)
    shared_part = narrow_product(shared_hidden, shared_down_weight) + narrow_product(
        down_middle, down_second
    )
    layer_part = (
        token_product(spread, (row_gate * expert_result.astype(jnp.float32)).astype(half))
        + shared_weight * shared_part
    )
    layer_sum = scatter_rows(layer_part)
    upstream_wide = upstream_all.astype(jnp.float32)
    shared_dot = jnp.sum(upstream_wide * shared_part, axis=1)

    upstream_rows = narrow_product(spread, upstream_all)
    row_dot = jnp.sum(upstream_rows * expert_result.astype(jnp.float32), axis=1, keepdims=True)
    gate_dot = jnp.sum(jnp.where(placed, row_dot, 0.0), axis=0)
    expert_upstream = (row_gate * upstream_rows).astype(half)
    expert_down_joined = jnp.concatenate([expert_down_weight[0], expert_down_second], axis=0)
    expert_grad_hidden = rows_product(expert_upstream, expert_down_joined)
    expert_down_inner = chosen(expert_grad_hidden[:, feed:], row_selector)
    expert_grad_hidden = expert_grad_hidden[:, :feed] + rows_product(
        expert_down_inner, expert_down_first
    )
    expert_grad_pre = gated_back(expert_pre[0], expert_pre[1], expert_grad_hidden)
    expert_inner = chosen(rows_product(expert_grad_pre, expert_up), twice(row_selector))
    copy_grad = rows_product(
        jnp.concatenate([expert_grad_pre, expert_inner], axis=1), expert_joined
    ).astype(half)

    value_grads = (shared_weight * upstream_wide).astype(half)
    down_joined = jnp.concatenate([shared_down_weight, down_second], axis=0)
    shared_grad_hidden = rows_product(value_grads, down_joined)
    down_inner = chosen(shared_grad_hidden[:, shared_wide:], selector)
    shared_grad_hidden = shared_grad_hidden[:, :shared_wide] + rows_product(down_inner, down_first)
    shared_grad_pre = gated_back(shared_pre[0], shared_pre[1], shared_grad_hidden)
    shared_inner = chosen(rows_product(shared_grad_pre, shared_up), twice(selector))
    second_part = token_product(spread, copy_grad) + rows_product(
        jnp.concatenate([shared_grad_pre, shared_inner], axis=1), shared_joined
    )
    dots = jnp.concatenate(
        [
            jnp.where(expert_range[:, None] == owner_index, gate_dot[None, :], 0.0),
            shared_dot[None, :],
            jnp.zeros((7, group_rows), jnp.float32),
        ],
        axis=0,
    )
    dots = jnp.transpose(dots.reshape(dots.shape[0], owners, count_rows), (1, 0, 2))
    own_dots = jnp.transpose(
        jnp.sum(lax.all_to_all(dots, "expert", split_axis=0, concat_axis=0, tiled=True), axis=0)
    )
    second_part, layer_sum = lax.optimization_barrier((second_part.astype(half), layer_sum))
    second_sum = scatter_rows(second_part).astype(jnp.float32)
    own_weights = own_rows(gate_weights)
    gate_grads = own_dots[:, :experts]
    centered = own_weights * (
        gate_grads - jnp.sum(own_weights * gate_grads, axis=1, keepdims=True)
    )
    logit_grads = centered.astype(half)
    own_selector = None if selector is None else own_rows(selector)
    router_inner = chosen(rows_product(logit_grads, router_second), own_selector)
    own_shared_weight = own_rows(shared_weight)
    weight_grads = own_dots[:, experts : experts + 1] * own_shared_weight * (1.0 - own_shared_weight)
    second_grad = (
        second_sum
        + rows_product(logit_grads, router_projection)
        + rows_product(router_inner, router_first)
        + weight_grads * shared_gate_vector.astype(jnp.float32)[None, :]
    )
    residual_grad = cotangent.astype(jnp.float32) + rms_backward(
        residual_stream, factor_second, experts_norm_gain, second_grad
    )
    output_upstream = slot_rows(
        lax.all_gather(residual_grad.astype(half), "expert", axis=0, tiled=True)
    )

    wide_grads = jnp.concatenate(
        [
            *row_blocks(token_product(expert_inner, expert_rows), 2),
            *diagonal_blocks(token_product(expert_middle, expert_grad_pre), 2),
            token_product(expert_down_inner, expert_hidden),
            token_product(expert_down_middle, expert_upstream),
            jnp.broadcast_to(
                jnp.repeat(adapter_slot_index, ADAPTER_RANK).astype(jnp.float32)[:, None],
                (slot_count * ADAPTER_RANK, 128),
            ),
        ],
        axis=1,
    ).astype(half)
    wide_grads, output_upstream = lax.optimization_barrier((wide_grads, output_upstream))
    expert_grads = lax.all_gather(wide_grads, "dp", axis=0, tiled=True)

    output_inner = rows_product(output_upstream, output_second).astype(half)
    attended_grad = (
        rows_product(output_upstream, output_weight) + rows_product(output_inner, output_first)
    ).astype(half)
    pre_grads = jnp.concatenate(
        head_attention_back(
            query_low,
            key_low,
            value_low,
            attended_grad,
            length,
            cosine_table,
            sine_table,
            score_scale,
        ),
        axis=1,
    )
    pre_grads, expert_grads = lax.optimization_barrier((pre_grads, expert_grads))
    qkv_inner = rows_product(pre_grads, qkv_up).astype(half)
    first_part = rows_product(jnp.concatenate([pre_grads, qkv_inner], axis=1), qkv_joined)
    first_part = group_wide(first_part).astype(half)
    layer_out = (residual_stream + layer_sum.astype(jnp.float32)).astype(half)

    own_router_middle = own_rows(router_middle)
    router_grad_b = token_product(own_router_middle, logit_grads)
    spare = -experts % 128
    summed, owned, first_part = reduce_adapters(
        [slot_wide(value) for value in row_blocks(token_product(qkv_inner, first_narrow), 3)]
        + [slot_wide(token_product(output_middle, output_upstream))]
        + row_blocks(token_product(shared_inner, second_all), 2)
        + [
            token_product(down_middle, value_grads),
            token_product(router_inner, second_own),
            jnp.pad(router_grad_b, ((0, 0), (0, spare))),
        ],
        [
            slot_wide(value)
            for value in diagonal_blocks(token_product(attention_middle, pre_grads), 3)
        ]
        + [slot_wide(token_product(output_inner, attended_low))]
        + diagonal_blocks(token_product(shared_middle, shared_grad_pre), 2)
        + [token_product(down_inner, shared_hidden)],
        [head_column] * 4 + [owner_index * shared_wide] * 3,
        [model_width_size] * 4 + [owners * shared_wide] * 3,
        adapter_slot_index,
        owner_index,
        owners,
        first_part,
    )
    first_grad = scatter_rows(first_part).astype(jnp.float32)
    unused, factor_first = rms_forward(input_rows, attention_norm_gain)
    tokens_grad = residual_grad + rms_backward(
        input_rows, factor_first, attention_norm_gain, first_grad
    )
    attn_grad_a = jnp.stack([jnp.transpose(value) for value in summed[:3] + owned[3:4]])
    attn_grad_b = jnp.stack(owned[:3] + summed[3:4])

    rank_range = jnp.arange(ADAPTER_COUNT * ADAPTER_RANK, dtype=jnp.int32)
    source_rank = jnp.arange(expert_grads.shape[0], dtype=jnp.int32)
    source_place = expert_grads[:, -1].astype(jnp.int32) * ADAPTER_RANK + source_rank % ADAPTER_RANK
    placement = (source_place[:, None] == rank_range[None, :]).astype(half)
    bounds = [0, model_width_size, 2 * model_width_size]
    bounds += [bounds[-1] + feed, bounds[-1] + 2 * feed, bounds[-1] + 3 * feed]
    expert_pieces = [
        expert_grads[:, start:stop] for start, stop in zip(bounds, bounds[1:] + [expert_grads.shape[1] - 128])
    ]
    in_grad_a = jnp.stack([token_product(value, placement) for value in expert_pieces[:2]])
    in_grad_b = jnp.stack([token_product(placement, value) for value in expert_pieces[2:4]])
    down_grad_a = token_product(expert_pieces[4], placement)
    down_grad_b = token_product(placement, expert_pieces[5])
    return (
        layer_out,
        tokens_grad,
        attn_grad_a,
        attn_grad_b,
        jnp.transpose(summed[7]),
        summed[8][:, :experts],
        jnp.stack([jnp.transpose(summed[4]), jnp.transpose(summed[5])]),
        jnp.stack(owned[4:6]),
        jnp.transpose(owned[6]),
        summed[6],
        in_grad_a[None],
        in_grad_b[None],
        down_grad_a[None],
        down_grad_b[None],
    )


def solution(mesh):
    return jax.shard_map(
        on_device,
        mesh=mesh,
        in_specs=(
            P(("dp", "expert"), None),
            P(("dp", "expert"), None),
            P(),
            P(),
            P(None, "expert"),
            P("expert", None),
            P(),
            P(None, None, "expert"),
            P("expert", None),
            P(),
            P("expert", None, None, None),
            P("expert", None, None),
            P(("dp", "expert"), None),
            P("dp"),
            P("dp"),
            P(),
            P(),
            P(),
            P(),
            P(),
            P(),
            P(),
            P(),
            P("expert", None, None, None),
            P("expert", None, None, None),
            P("expert", None, None),
            P("expert", None, None),
        ),
        out_specs=(
            P(("dp", "expert"), None),
            P(("dp", "expert"), None),
            P(None, None, ("dp", "expert")),
            P(None, ("dp", "expert"), None),
            P(None, ("dp", "expert")),
            P(("dp", "expert"), None),
            P(None, None, ("dp", "expert")),
            P(None, ("dp", "expert"), None),
            P(None, ("dp", "expert")),
            P(("dp", "expert"), None),
            P("expert", None, None, None),
            P("expert", None, None, None),
            P("expert", None, None),
            P("expert", None, None),
        ),
        check_vma=False,
    )
```

```python
import functools
import math

import jax
import jax.numpy as jnp
from jax import lax
from jax.experimental import pallas as pl
from jax.experimental.pallas import tpu as pltpu
from jax.sharding import PartitionSpec as P

HEADS = 16
HEAD_DIM = 128
ADAPTER_RANK = 16
ADAPTER_COUNT = 8
BLOCK = 256
SEQ_MAX = 2048


NORM_EPS = 1e-06
ROPE_BASE = 1000000.0
MASKED = -1e30


def narrow_product(left_side, right_side):
    return jnp.dot(left_side, right_side, preferred_element_type=jnp.float32)


def rms_forward(values, gain_vector):
    factor = lax.rsqrt(jnp.mean(values * values, axis=-1, keepdims=True) + NORM_EPS)
    return (values * factor * gain_vector, factor)


def rms_backward(values, factor, gain_vector, upstream):
    weighted = upstream * gain_vector
    return factor * weighted - values * (factor * factor * factor) * jnp.mean(
        values * weighted, axis=-1, keepdims=True
    )


def rope_tables(positions, head_width):
    half_width = head_width // 2
    inverse = ROPE_BASE ** (-(jnp.arange(half_width).astype(jnp.float32) * 2.0 / head_width))
    angles = positions.astype(jnp.float32)[:, None] * inverse[None, :]
    return (jnp.cos(angles), jnp.sin(angles))


def turn(values, cosine_table, sine_table):
    return values * cosine_table + pltpu.roll(values, HEAD_DIM // 2, 1) * sine_table


def head_product(left_side, right_side, left_dim, right_dim):
    return lax.dot_general(
        left_side,
        right_side,
        (((left_dim,), (right_dim,)), ((), ())),
        preferred_element_type=jnp.float32,
    )


def block_probabilities(query_rows, key_rows, live, score_scale):
    scores = head_product(query_rows, key_rows, 1, 1) * score_scale
    scores = jnp.where(live, scores, MASKED)
    exponents = jnp.exp(scores - jnp.max(scores, axis=1, keepdims=True))
    return exponents / jnp.sum(exponents, axis=1, keepdims=True)


def attention_forward(
    score_scale, length_ref, q_ref, k_ref, v_ref, cos_ref, sin_ref, out_ref, ql_ref, kl_ref, vl_ref
):
    rows = q_ref.shape[0]
    cosine_table, sine_table = cos_ref[...], sin_ref[...]
    ql_ref[...] = turn(q_ref[...], cosine_table, sine_table).astype(jnp.bfloat16)
    kl_ref[...] = turn(k_ref[...], cosine_table, sine_table).astype(jnp.bfloat16)
    vl_ref[...] = v_ref[...].astype(jnp.bfloat16)
    for start in range(0, rows, BLOCK):
        stop = start + BLOCK
        live = lax.broadcasted_iota(jnp.int32, (BLOCK, stop), 1) < length_ref[0]
        probabilities = block_probabilities(
            ql_ref[start:stop, :], kl_ref[:stop, :], live, score_scale
        )
        out_ref[start:stop, :] = head_product(
            probabilities.astype(jnp.bfloat16), vl_ref[:stop, :], 1, 0
        ).astype(jnp.bfloat16)


def attention_backward(
    score_scale,
    length_ref,
    q_ref,
    k_ref,
    v_ref,
    grad_ref,
    cos_ref,
    sin_ref,
    dq_ref,
    dk_ref,
    dv_ref,
    key_sum,
    value_sum,
):
    rows = q_ref.shape[0]
    cosine_table, sine_table = cos_ref[...], sin_ref[...]
    key_sum[...] = jnp.zeros_like(key_sum)
    value_sum[...] = jnp.zeros_like(value_sum)
    for start in range(0, rows, BLOCK):
        stop = start + BLOCK
        live = lax.broadcasted_iota(jnp.int32, (BLOCK, stop), 1) < length_ref[0]
        query_rows, grad_rows = q_ref[start:stop, :], grad_ref[start:stop, :]
        probabilities = block_probabilities(query_rows, k_ref[:stop, :], live, score_scale)
        narrow = probabilities.astype(jnp.bfloat16)
        prob_grads = head_product(grad_rows, v_ref[:stop, :], 1, 1)
        delta = jnp.sum(narrow.astype(jnp.float32) * prob_grads, axis=1, keepdims=True)
        score_grads = (probabilities * (prob_grads - delta)).astype(jnp.bfloat16)
        query_grads = head_product(score_grads, k_ref[:stop, :], 1, 0) * score_scale
        dq_ref[start:stop, :] = turn(
            query_grads, cosine_table[start:stop, :], -sine_table[start:stop, :]
        ).astype(jnp.bfloat16)
        key_sum[:stop, :] += head_product(score_grads, query_rows, 0, 0)
        value_sum[:stop, :] += head_product(narrow, grad_rows, 0, 0)
    dk_ref[...] = turn(key_sum[...] * score_scale, cosine_table, -sine_table).astype(jnp.bfloat16)
    dv_ref[...] = value_sum[...].astype(jnp.bfloat16)


def head_attention(query, key, value, length, cosine_table, sine_table, score_scale):
    rows, width = query.shape
    head = pl.BlockSpec((rows, HEAD_DIM), lambda place: (0, place))
    table = pl.BlockSpec((rows, HEAD_DIM), lambda place: (0, 0))
    shape = jax.ShapeDtypeStruct((rows, width), jnp.bfloat16)
    return pl.pallas_call(
        functools.partial(attention_forward, score_scale),
        grid=(width // HEAD_DIM,),
        in_specs=[pl.BlockSpec(memory_space=pltpu.SMEM), head, head, head, table, table],
        out_specs=[head] * 4,
        out_shape=[shape] * 4,
        compiler_params=pltpu.CompilerParams(vmem_limit_bytes=48 * 1024 * 1024),
        cost_estimate=pl.CostEstimate(
            flops=3 * rows * rows * width, bytes_accessed=24 * rows * width, transcendentals=rows * rows
        ),
        name="head_attention",
    )(length, query, key, value, cosine_table, sine_table)


def head_attention_back(query, key, value, grad, length, cosine_table, sine_table, score_scale):
    rows, width = query.shape
    head = pl.BlockSpec((rows, HEAD_DIM), lambda place: (0, place))
    table = pl.BlockSpec((rows, HEAD_DIM), lambda place: (0, 0))
    shape = jax.ShapeDtypeStruct((rows, width), jnp.bfloat16)
    return pl.pallas_call(
        functools.partial(attention_backward, score_scale),
        grid=(width // HEAD_DIM,),
        in_specs=[pl.BlockSpec(memory_space=pltpu.SMEM)] + [head] * 4 + [table, table],
        out_specs=[head] * 3,
        out_shape=[shape] * 3,
        scratch_shapes=[
            pltpu.VMEM((rows, HEAD_DIM), jnp.float32),
            pltpu.VMEM((rows, HEAD_DIM), jnp.float32),
        ],
        compiler_params=pltpu.CompilerParams(vmem_limit_bytes=48 * 1024 * 1024),
        cost_estimate=pl.CostEstimate(
            flops=7 * rows * rows * width, bytes_accessed=16 * rows * width, transcendentals=rows * rows
        ),
        name="head_attention_back",
    )(length, query, key, value, grad, cosine_table, sine_table)


def rows_product(left_side, right_side):
    return lax.dot_general(
        left_side, right_side, (((1,), (1,)), ((), ())), preferred_element_type=jnp.float32
    )


def token_product(left_side, right_side):
    return lax.dot_general(
        left_side, right_side, (((0,), (0,)), ((), ())), preferred_element_type=jnp.float32
    )


def joint_products(left_side, right_sides):
    product = narrow_product(left_side, jnp.concatenate(right_sides, axis=1))
    pieces, at = [], 0
    for value in right_sides:
        pieces.append(product[:, at : at + value.shape[1]])
        at += value.shape[1]
    return pieces


def block_diagonal(blocks):
    rows = []
    for place, value in enumerate(blocks):
        row = [
            value if other == place else jnp.zeros((value.shape[0], side.shape[1]), value.dtype)
            for other, side in enumerate(blocks)
        ]
        rows.append(jnp.concatenate(row, axis=1))
    return jnp.concatenate(rows, axis=0)


def diagonal_blocks(product, count):
    rows, columns = product.shape[0] // count, product.shape[1] // count
    return [
        product[place * rows : (place + 1) * rows, place * columns : (place + 1) * columns]
        for place in range(count)
    ]


def row_blocks(product, count):
    rows = product.shape[0] // count
    return [product[place * rows : (place + 1) * rows] for place in range(count)]


def gated_back(gate_value, up_value, grad_hidden):
    sigmoid_gate = jax.nn.sigmoid(gate_value)
    grad_gate = grad_hidden * up_value * sigmoid_gate * (1.0 + gate_value * (1.0 - sigmoid_gate))
    grad_up = grad_hidden * gate_value * sigmoid_gate
    return jnp.concatenate([grad_gate, grad_up], axis=1).astype(jnp.bfloat16)


def head_weights(columns, owner_index, owners, slot_count, head_start, width):
    model_width_size, held = columns.shape
    groups = lax.axis_size("dp")
    group_index = lax.axis_index("dp")
    if slot_count == 1 and held == 3 * width and owners % 3 and groups & (groups - 1) == 0:
        share = model_width_size // groups
        mine = lax.dynamic_slice_in_dim(columns, group_index * share, share, 0)
        moved = jnp.stack(
            [
                lax.ppermute(
                    mine[:, step * width : (step + 1) * width],
                    "expert",
                    [(source, (3 * source + step) % owners) for source in range(owners)],
                )
                for step in range(3)
            ]
        )
        kinds = jnp.stack(
            [
                lax.dynamic_index_in_dim(moved, (owner_index + owners * kind) % 3, 0, False)
                for kind in range(3)
            ]
        )
        shares = jnp.stack(
            [kinds]
            + [
                lax.ppermute(kinds, "dp", [(source, source ^ step) for source in range(groups)])
                for step in range(1, groups)
            ]
        )
        ordered = jnp.concatenate(
            [
                lax.dynamic_index_in_dim(shares, group_index ^ place, 0, False)
                for place in range(groups)
            ],
            axis=1,
        )
        return [ordered[kind] for kind in range(3)]
    full = lax.all_gather(columns, "expert", axis=1, tiled=True)
    return [
        lax.dynamic_slice_in_dim(full, kind * model_width_size + head_start * HEAD_DIM, width, 1)
        for kind in range(3)
    ]


def spread_adapters(compact, adapter_index):
    ranks = ADAPTER_COUNT * ADAPTER_RANK
    total = jnp.zeros((ranks, compact.shape[1]), compact.dtype)
    for slot in range(adapter_index.shape[0]):
        piece = compact[slot * ADAPTER_RANK : (slot + 1) * ADAPTER_RANK]
        total = total + lax.dynamic_update_slice_in_dim(
            jnp.zeros_like(total), piece, adapter_index[slot] * ADAPTER_RANK, 0
        )
    return total


def reduce_adapters(
    partial, owned, owned_starts, owned_totals, adapter_index, owner_index, owners, ahead
):
    groups = lax.axis_size("dp")
    group_index = lax.axis_index("dp")
    slot_count = adapter_index.shape[0]
    partial_sizes = [value.shape[1] for value in partial]
    owned_sizes = [value.shape[1] for value in owned]
    partial_all = jnp.concatenate(partial, axis=1)
    owned_all = jnp.concatenate(owned, axis=1)

    def cut(values, sizes):
        pieces, at = [], 0
        for size in sizes:
            pieces.append(values[..., at : at + size])
            at += size
        return pieces

    if slot_count > 1 or ADAPTER_RANK % owners or ADAPTER_COUNT % groups or owners % (
        ADAPTER_COUNT // groups
    ):
        wide = [
            lax.dynamic_update_slice_in_dim(
                jnp.zeros((value.shape[0], total), value.dtype), value, start, 1
            )
            for value, start, total in zip(owned, owned_starts, owned_totals)
        ]
        dense = spread_adapters(jnp.concatenate([partial_all] + wide, axis=1), adapter_index)
        summed = lax.psum_scatter(dense, ("dp", "expert"), scatter_dimension=0, tiled=True)
        pieces = cut(summed, partial_sizes + owned_totals)
        return pieces[: len(partial)], pieces[len(partial) :], ahead

    local = ADAPTER_COUNT // groups
    own_rows = ADAPTER_RANK // owners
    held = sum(partial_sizes)
    joined = jnp.concatenate([partial_all, owned_all], axis=1).astype(jnp.bfloat16)
    joined, ahead = lax.optimization_barrier((joined, ahead))
    moved = lax.all_to_all(
        joined.reshape(owners, own_rows, joined.shape[1]),
        "expert",
        split_axis=0,
        concat_axis=0,
        tiled=True,
    )
    scattered = jnp.sum(moved[:, :, :held].astype(jnp.float32), axis=0).astype(jnp.bfloat16)
    placed = [
        jnp.transpose(value, (1, 0, 2)).reshape(own_rows, owners * size)
        for value, size in zip(cut(moved[:, :, held:], owned_sizes), owned_sizes)
    ]
    label = jnp.broadcast_to(adapter_index[:, None], (own_rows, 128)).astype(jnp.bfloat16)
    gathered = lax.all_gather(
        jnp.concatenate([scattered] + placed + [label], axis=1), "dp", axis=0
    ).astype(jnp.float32)
    labels = gathered[:, :, -1:]
    gathered = gathered[:, :, :-128]
    sums = []
    for which in range(local):
        wanted = labels == (group_index * local + which).astype(jnp.float32)
        sums.append(jnp.sum(jnp.where(wanted, gathered, 0.0), axis=0))
    sums = jnp.stack(sums).astype(jnp.bfloat16)
    arrived = []
    for step in range(local):
        piece = lax.dynamic_index_in_dim(sums, (step + owner_index) % local, 0, False)
        arrived.append(
            lax.ppermute(
                piece,
                "expert",
                [
                    (source, (step + source) % local * (owners // local) + source // local)
                    for source in range(owners)
                ],
            )
        )
    arrived = jnp.stack(arrived)
    place = owner_index // (owners // local)
    rows = jnp.concatenate(
        [
            lax.dynamic_index_in_dim(arrived, (place - which) % local, 0, False)
            for which in range(local)
        ],
        axis=0,
    )
    pieces = cut(rows.astype(jnp.float32), partial_sizes + [owners * size for size in owned_sizes])
    return pieces[: len(partial)], pieces[len(partial) :], ahead


def on_device(
    tokens,
    cotangent,
    attention_norm_gain,
    experts_norm_gain,
    attention_query_key_value,
    attention_output_weight,
    router_projection,
    shared_gate_up_weight,
    shared_down_weight,
    shared_gate_vector,
    expert_gate_up_weight,
    expert_down_weight,
    routes,
    lengths,
    adapter_slot_index,
    attention_adapter_first,
    attention_adapter_second,
    router_adapter_first,
    router_adapter_second,
    shared_adapter_first,
    shared_adapter_second,
    shared_down_adapter_first,
    shared_down_adapter_second,
    expert_adapter_first,
    expert_adapter_second,
    expert_down_adapter_first,
    expert_down_adapter_second,
):
    count_rows, model_width_size = tokens.shape
    owners = lax.axis_size("expert")
    owner_index = lax.axis_index("expert")
    experts = router_projection.shape[1]
    top_count = routes.shape[1]
    capacity = (count_rows * top_count * 9 + 8 * experts - 1) // (8 * experts)
    group_rows = count_rows * owners
    seq_length = min(SEQ_MAX, group_rows)
    slot_count = lengths.shape[0]
    group_devices = owners // slot_count
    head_count = HEADS // group_devices
    width = head_count * HEAD_DIM
    own_slot = owner_index // group_devices
    head_start = owner_index % group_devices * head_count
    head_column = head_start * HEAD_DIM
    score_scale = 1.0 / math.sqrt(HEAD_DIM)
    half = jnp.bfloat16

    def own_rows(values):
        return lax.dynamic_slice_in_dim(values, owner_index * count_rows, count_rows, 0)

    def slot_rows(values):
        if slot_count == 1:
            return values
        return lax.dynamic_slice_in_dim(values, own_slot * seq_length, seq_length, 0)

    def group_wide(values):
        if slot_count == 1:
            return values
        return lax.dynamic_update_slice_in_dim(
            jnp.zeros((group_rows, values.shape[1]), values.dtype), values, own_slot * seq_length, 0
        )

    def slot_wide(values):
        if slot_count == 1:
            return values
        return lax.dynamic_update_slice_in_dim(
            jnp.zeros((slot_count * ADAPTER_RANK, values.shape[1]), values.dtype),
            values,
            own_slot * ADAPTER_RANK,
            0,
        )

    def slot_value(values):
        return values[0] if slot_count == 1 else lax.dynamic_index_in_dim(values, own_slot, 0, False)

    def picked_maps(maps, axis):
        return jnp.concatenate(
            [
                lax.dynamic_slice_in_dim(
                    maps, adapter_slot_index[slot] * ADAPTER_RANK, ADAPTER_RANK, axis
                )
                for slot in range(slot_count)
            ],
            axis=axis,
        )

    def scatter_rows(values):
        return lax.psum_scatter(values.astype(half), "expert", scatter_dimension=0, tiled=True)

    tokens_all = lax.all_gather(tokens, "expert", axis=0, tiled=True)
    qkv_weights = head_weights(
        attention_query_key_value, owner_index, owners, slot_count, head_start, width
    )
    routes_all = lax.all_gather(routes, "expert", axis=0, tiled=True)
    upstream_all = lax.all_gather(cotangent, "expert", axis=0, tiled=True)
    if attention_output_weight.shape[0] == width:
        output_weight = attention_output_weight
    else:
        output_weight = lax.dynamic_slice_in_dim(
            lax.all_gather(attention_output_weight, "expert", axis=0, tiled=True),
            head_column,
            width,
            0,
        )

    if slot_count == 1:
        selector = None
    else:
        row_slot = jnp.arange(group_rows, dtype=jnp.int32) // seq_length
        rank_slot = jnp.arange(slot_count * ADAPTER_RANK, dtype=jnp.int32) // ADAPTER_RANK
        selector = (row_slot[:, None] == rank_slot[None, :]).astype(half)

    def chosen(values, picker):
        narrow = values.astype(half)
        return narrow if picker is None else narrow * picker

    def twice(picker):
        return None if picker is None else jnp.concatenate([picker, picker], axis=1)

    attention_adapter = slot_value(adapter_slot_index) * ADAPTER_RANK
    attention_first = lax.dynamic_slice_in_dim(
        attention_adapter_first, attention_adapter, ADAPTER_RANK, 2
    )
    attention_second = lax.dynamic_slice_in_dim(
        attention_adapter_second, attention_adapter, ADAPTER_RANK, 1
    )
    qkv_second = lax.dynamic_slice_in_dim(attention_second[:3], head_column, width, 2)
    output_first = lax.dynamic_slice_in_dim(attention_first[3], head_column, width, 0)
    output_second = attention_second[3]
    router_first = picked_maps(router_adapter_first, 1)
    router_second = picked_maps(router_adapter_second, 0)
    shared_wide = shared_down_weight.shape[0]
    shared_first = picked_maps(shared_adapter_first, 2)
    shared_second = lax.dynamic_slice_in_dim(
        picked_maps(shared_adapter_second, 1), owner_index * shared_wide, shared_wide, 2
    )
    down_first = lax.dynamic_slice_in_dim(
        picked_maps(shared_down_adapter_first, 1), owner_index * shared_wide, shared_wide, 0
    )
    down_second = picked_maps(shared_down_adapter_second, 0)
    expert_first = picked_maps(expert_adapter_first[0], 2)
    expert_second = picked_maps(expert_adapter_second[0], 1)
    expert_down_first = picked_maps(expert_down_adapter_first[0], 1)
    expert_down_second = picked_maps(expert_down_adapter_second[0], 0)

    expert_joined = jnp.concatenate(
        [expert_gate_up_weight[0, 0], expert_gate_up_weight[0, 1], expert_first[0], expert_first[1]],
        axis=1,
    )
    shared_joined = jnp.concatenate(
        [shared_gate_up_weight[0], shared_gate_up_weight[1], shared_first[0], shared_first[1]], axis=1
    )
    expert_down_joined = jnp.concatenate([expert_down_weight[0], expert_down_second], axis=0)
    down_joined = jnp.concatenate([shared_down_weight, down_second], axis=0)
    tokens_all, routes_all, expert_joined, shared_joined, expert_down_joined, down_joined = (
        lax.optimization_barrier(
            (
                tokens_all,
                routes_all,
                expert_joined,
                shared_joined,
                expert_down_joined,
                down_joined,
            )
        )
    )

    expert_range = jnp.arange(experts, dtype=jnp.int32)
    route_hits = jnp.any(routes_all[:, :, None] == expert_range[None, None, :], axis=1)
    own_hits = jnp.any(routes_all == owner_index, axis=1)
    ranks = jnp.cumsum(own_hits.astype(jnp.int32)) - 1
    row_range = jnp.arange(experts * capacity, dtype=jnp.int32)
    placed = (ranks[None, :] == row_range[:, None]) & own_hits[None, :]
    spread = placed.astype(half)
    row_selector = None if selector is None else narrow_product(spread, selector).astype(half)

    slot_tokens = slot_rows(tokens_all).astype(jnp.float32)
    normed_first, unused = rms_forward(slot_tokens, attention_norm_gain)
    first_narrow = normed_first.astype(half)
    positions = jnp.arange(seq_length, dtype=jnp.int32)
    cosine_table, sine_table = rope_tables(positions, HEAD_DIM)
    cosine_table = jnp.concatenate([cosine_table, cosine_table], axis=1)
    sine_table = jnp.concatenate([-sine_table, sine_table], axis=1)
    length = slot_value(lengths).reshape(1)
    first_narrow, qkv_weights = lax.optimization_barrier((first_narrow, qkv_weights))
    qkv_joined = jnp.concatenate(qkv_weights + [attention_first[kind] for kind in range(3)], axis=1)
    qkv_up = block_diagonal([qkv_second[kind] for kind in range(3)])
    projected = narrow_product(first_narrow, qkv_joined)
    attention_middle = projected[:, 3 * width :].astype(half)
    projected = projected[:, : 3 * width] + narrow_product(attention_middle, qkv_up)
    projected = [projected[:, kind * width : (kind + 1) * width] for kind in range(3)]
    attended_low, query_low, key_low, value_low = head_attention(
        *projected, length, cosine_table, sine_table, score_scale
    )
    attended_low, upstream_all = lax.optimization_barrier((attended_low, upstream_all))
    output_middle = narrow_product(attended_low, output_first).astype(half)
    attention_part = narrow_product(attended_low, output_weight) + narrow_product(
        output_middle, output_second
    )
    input_rows = tokens.astype(jnp.float32)
    residual_stream = input_rows + scatter_rows(group_wide(attention_part)).astype(jnp.float32)
    normed_second, factor_second = rms_forward(residual_stream, experts_norm_gain)
    second_own = normed_second.astype(half)
    second_all = lax.all_gather(second_own, "expert", axis=0, tiled=True)

    router_raw, router_plain, gate_raw = joint_products(
        second_all, [router_first, router_projection, shared_gate_vector[:, None]]
    )
    router_middle = chosen(router_raw, selector)
    router_scores = router_plain + narrow_product(router_middle, router_second)
    reach = jnp.max(jnp.where(route_hits, router_scores, MASKED), axis=1, keepdims=True)
    gate_exponents = jnp.where(route_hits, jnp.exp(jnp.minimum(router_scores - reach, 0.0)), 0.0)
    gate_weights = gate_exponents / jnp.sum(gate_exponents, axis=1, keepdims=True)
    own_gate = jnp.sum(jnp.where(expert_range[None, :] == owner_index, gate_weights, 0.0), axis=1)
    row_gate = jnp.sum(jnp.where(placed, own_gate[None, :], 0.0), axis=1, keepdims=True)
    shared_weight = jax.nn.sigmoid(gate_raw)

    expert_rows = narrow_product(spread, second_all).astype(half)
    feed = expert_down_weight.shape[1]
    expert_up = block_diagonal([expert_second[0], expert_second[1]])
    expert_pre = narrow_product(expert_rows, expert_joined)
    expert_middle = chosen(expert_pre[:, 2 * feed :], twice(row_selector))
    expert_pre = expert_pre[:, : 2 * feed] + narrow_product(expert_middle, expert_up)
    expert_pre = (expert_pre[:, :feed], expert_pre[:, feed:])
    expert_hidden = (jax.nn.silu(expert_pre[0]) * expert_pre[1]).astype(half)
    expert_down_middle = chosen(narrow_product(expert_hidden, expert_down_first), row_selector)
    expert_result = (
        narrow_product(expert_hidden, expert_down_weight[0])
        + narrow_product(expert_down_middle, expert_down_second)
    ).astype(half)

    shared_up = block_diagonal([shared_second[0], shared_second[1]])
    shared_pre = narrow_product(second_all, shared_joined)
    shared_middle = chosen(shared_pre[:, 2 * shared_wide :], twice(selector))
    shared_pre = shared_pre[:, : 2 * shared_wide] + narrow_product(shared_middle, shared_up)
    shared_pre = (shared_pre[:, :shared_wide], shared_pre[:, shared_wide:])
    shared_hidden = (jax.nn.silu(shared_pre[0]) * shared_pre[1]).astype(half)
    down_middle = chosen(narrow_product(shared_hidden, down_first), selector)
    shared_part = narrow_product(shared_hidden, shared_down_weight) + narrow_product(
        down_middle, down_second
    )
    layer_part = (
        token_product(spread, (row_gate * expert_result.astype(jnp.float32)).astype(half))
        + shared_weight * shared_part
    )
    layer_sum = scatter_rows(layer_part)
    upstream_wide = upstream_all.astype(jnp.float32)
    shared_dot = jnp.sum(upstream_wide * shared_part, axis=1)

    upstream_rows = narrow_product(spread, upstream_all)
    row_dot = jnp.sum(upstream_rows * expert_result.astype(jnp.float32), axis=1, keepdims=True)
    gate_dot = jnp.sum(jnp.where(placed, row_dot, 0.0), axis=0)
    expert_upstream = (row_gate * upstream_rows).astype(half)
    expert_grad_hidden = rows_product(expert_upstream, expert_down_joined)
    expert_down_inner = chosen(expert_grad_hidden[:, feed:], row_selector)
    expert_grad_hidden = expert_grad_hidden[:, :feed] + rows_product(
        expert_down_inner, expert_down_first
    )
    expert_grad_pre = gated_back(expert_pre[0], expert_pre[1], expert_grad_hidden)
    expert_inner = chosen(rows_product(expert_grad_pre, expert_up), twice(row_selector))
    expert_grad_joined = lax.optimization_barrier(
        jnp.concatenate([expert_grad_pre, expert_inner], axis=1)
    )
    copy_grad = rows_product(expert_grad_joined, expert_joined).astype(half)

    value_grads = (shared_weight * upstream_wide).astype(half)
    shared_grad_hidden = rows_product(value_grads, down_joined)
    down_inner = chosen(shared_grad_hidden[:, shared_wide:], selector)
    shared_grad_hidden = shared_grad_hidden[:, :shared_wide] + rows_product(down_inner, down_first)
    shared_grad_pre = gated_back(shared_pre[0], shared_pre[1], shared_grad_hidden)
    shared_inner = chosen(rows_product(shared_grad_pre, shared_up), twice(selector))
    shared_grad_joined = lax.optimization_barrier(
        jnp.concatenate([shared_grad_pre, shared_inner], axis=1)
    )
    second_part = token_product(spread, copy_grad) + rows_product(
        shared_grad_joined, shared_joined
    )
    dots = jnp.concatenate(
        [
            jnp.where(expert_range[:, None] == owner_index, gate_dot[None, :], 0.0),
            shared_dot[None, :],
            jnp.zeros((7, group_rows), jnp.float32),
        ],
        axis=0,
    )
    dots = jnp.transpose(dots.reshape(dots.shape[0], owners, count_rows), (1, 0, 2))
    own_dots = jnp.transpose(
        jnp.sum(lax.all_to_all(dots, "expert", split_axis=0, concat_axis=0, tiled=True), axis=0)
    )
    second_part, layer_sum = lax.optimization_barrier((second_part.astype(half), layer_sum))
    second_sum = scatter_rows(second_part).astype(jnp.float32)
    own_weights = own_rows(gate_weights)
    gate_grads = own_dots[:, :experts]
    centered = own_weights * (
        gate_grads - jnp.sum(own_weights * gate_grads, axis=1, keepdims=True)
    )
    logit_grads = centered.astype(half)
    own_selector = None if selector is None else own_rows(selector)
    router_inner = chosen(rows_product(logit_grads, router_second), own_selector)
    own_shared_weight = own_rows(shared_weight)
    weight_grads = own_dots[:, experts : experts + 1] * own_shared_weight * (1.0 - own_shared_weight)
    second_grad = (
        second_sum
        + rows_product(logit_grads, router_projection)
        + rows_product(router_inner, router_first)
        + weight_grads * shared_gate_vector.astype(jnp.float32)[None, :]
    )
    residual_grad = cotangent.astype(jnp.float32) + rms_backward(
        residual_stream, factor_second, experts_norm_gain, second_grad
    )
    output_upstream = slot_rows(
        lax.all_gather(residual_grad.astype(half), "expert", axis=0, tiled=True)
    )

    wide_grads = jnp.concatenate(
        [
            *row_blocks(token_product(expert_inner, expert_rows), 2),
            *diagonal_blocks(token_product(expert_middle, expert_grad_pre), 2),
            token_product(expert_down_inner, expert_hidden),
            token_product(expert_down_middle, expert_upstream),
            jnp.broadcast_to(
                jnp.repeat(adapter_slot_index, ADAPTER_RANK).astype(jnp.float32)[:, None],
                (slot_count * ADAPTER_RANK, 128),
            ),
        ],
        axis=1,
    ).astype(half)
    groups = lax.axis_size("dp")
    if groups & (groups - 1):
        expert_grads = lax.all_gather(wide_grads, "dp", axis=0, tiled=True)
    else:
        expert_grads = jnp.concatenate(
            [wide_grads]
            + [
                lax.ppermute(wide_grads, "dp", [(source, source ^ step) for source in range(groups)])
                for step in range(1, groups)
            ],
            axis=0,
        )

    output_inner = rows_product(output_upstream, output_second).astype(half)
    attended_grad = (
        rows_product(output_upstream, output_weight) + rows_product(output_inner, output_first)
    ).astype(half)
    pre_grads = jnp.concatenate(
        head_attention_back(
            query_low,
            key_low,
            value_low,
            attended_grad,
            length,
            cosine_table,
            sine_table,
            score_scale,
        ),
        axis=1,
    )
    pre_grads, expert_grads = lax.optimization_barrier((pre_grads, expert_grads))
    qkv_inner = rows_product(pre_grads, qkv_up).astype(half)
    first_part = rows_product(jnp.concatenate([pre_grads, qkv_inner], axis=1), qkv_joined)
    first_part = group_wide(first_part).astype(half)
    layer_out = (residual_stream + layer_sum.astype(jnp.float32)).astype(half)

    own_router_middle = own_rows(router_middle)
    router_grad_b = token_product(own_router_middle, logit_grads)
    spare = -experts % 128
    summed, owned, first_part = reduce_adapters(
        [slot_wide(value) for value in row_blocks(token_product(qkv_inner, first_narrow), 3)]
        + [slot_wide(token_product(output_middle, output_upstream))]
        + row_blocks(token_product(shared_inner, second_all), 2)
        + [
            token_product(down_middle, value_grads),
            token_product(router_inner, second_own),
            jnp.pad(router_grad_b, ((0, 0), (0, spare))),
        ],
        [
            slot_wide(value)
            for value in diagonal_blocks(token_product(attention_middle, pre_grads), 3)
        ]
        + [slot_wide(token_product(output_inner, attended_low))]
        + diagonal_blocks(token_product(shared_middle, shared_grad_pre), 2)
        + [token_product(down_inner, shared_hidden)],
        [head_column] * 4 + [owner_index * shared_wide] * 3,
        [model_width_size] * 4 + [owners * shared_wide] * 3,
        adapter_slot_index,
        owner_index,
        owners,
        first_part,
    )
    first_grad = scatter_rows(first_part).astype(jnp.float32)
    unused, factor_first = rms_forward(input_rows, attention_norm_gain)
    tokens_grad = residual_grad + rms_backward(
        input_rows, factor_first, attention_norm_gain, first_grad
    )
    attn_grad_a = jnp.stack([jnp.transpose(value) for value in summed[:3] + owned[3:4]])
    attn_grad_b = jnp.stack(owned[:3] + summed[3:4])

    rank_range = jnp.arange(ADAPTER_COUNT * ADAPTER_RANK, dtype=jnp.int32)
    source_rank = jnp.arange(expert_grads.shape[0], dtype=jnp.int32)
    source_place = expert_grads[:, -1].astype(jnp.int32) * ADAPTER_RANK + source_rank % ADAPTER_RANK
    placement = (source_place[:, None] == rank_range[None, :]).astype(half)
    bounds = [0, model_width_size, 2 * model_width_size]
    bounds += [bounds[-1] + feed, bounds[-1] + 2 * feed, bounds[-1] + 3 * feed]
    expert_pieces = [
        expert_grads[:, start:stop] for start, stop in zip(bounds, bounds[1:] + [expert_grads.shape[1] - 128])
    ]
    in_grad_a = jnp.stack([token_product(value, placement) for value in expert_pieces[:2]])
    in_grad_b = jnp.stack([token_product(placement, value) for value in expert_pieces[2:4]])
    down_grad_a = token_product(expert_pieces[4], placement)
    down_grad_b = token_product(placement, expert_pieces[5])
    return (
        layer_out,
        tokens_grad,
        attn_grad_a,
        attn_grad_b,
        jnp.transpose(summed[7]),
        summed[8][:, :experts],
        jnp.stack([jnp.transpose(summed[4]), jnp.transpose(summed[5])]),
        jnp.stack(owned[4:6]),
        jnp.transpose(owned[6]),
        summed[6],
        in_grad_a[None],
        in_grad_b[None],
        down_grad_a[None],
        down_grad_b[None],
    )


def solution(mesh):
    return jax.shard_map(
        on_device,
        mesh=mesh,
        in_specs=(
            P(("dp", "expert"), None),
            P(("dp", "expert"), None),
            P(),
            P(),
            P(None, "expert"),
            P("expert", None),
            P(),
            P(None, None, "expert"),
            P("expert", None),
            P(),
            P("expert", None, None, None),
            P("expert", None, None),
            P(("dp", "expert"), None),
            P("dp"),
            P("dp"),
            P(),
            P(),
            P(),
            P(),
            P(),
            P(),
            P(),
            P(),
            P("expert", None, None, None),
            P("expert", None, None, None),
            P("expert", None, None),
            P("expert", None, None),
        ),
        out_specs=(
            P(("dp", "expert"), None),
            P(("dp", "expert"), None),
            P(None, None, ("dp", "expert")),
            P(None, ("dp", "expert"), None),
            P(None, ("dp", "expert")),
            P(("dp", "expert"), None),
            P(None, None, ("dp", "expert")),
            P(None, ("dp", "expert"), None),
            P(None, ("dp", "expert")),
            P(("dp", "expert"), None),
            P("expert", None, None, None),
            P("expert", None, None, None),
            P("expert", None, None),
            P("expert", None, None),
        ),
        check_vma=False,
    )
```
